256 devices in a mesh: groups: 2 (over y), row: 16 (over z), col: 4 (over x), sub: 2 (over core).
Axes of the slice: x: 4, y: 2, z: 16, core: 2. Of those that a mesh axis runs over, the one named last changes fastest.
The devices are a block of a 4x16x16 slice.
Arguments:
- saved_alignment: bfloat16 [64, 1024, 256], P(('col', 'sub'), ('groups', 'row')), parts along dimension 1, may hold values from -6 to 6
- homolog_existence: int32 [64, 1024], P(('col', 'sub'), ('groups', 'row')), parts along dimension 1, may hold values 0 or 1
- amino_existence: int32 [1024], P(('groups', 'row')), parts along dimension 0, may hold values 0 or 1
- couple_delta_adjoint: bfloat16 [1024, 512, 128], P(('groups', 'row'), ('col', 'sub')), parts along dimension 0, may hold values from -1.5 to 1.5
- feedforward_adjoint: bfloat16 [64, 1024, 256], P(('col', 'sub'), ('groups', 'row')), parts along dimension 1, may hold values from -1.5 to 1.5
- feedforward_scale: float32 [256], replicated, may hold values from 0.1 to 1.9
- expansion_matrix: bfloat16 [256, 1024], replicated, may hold values from -0.375 to 0.375
- contraction_matrix: bfloat16 [1024, 256], replicated, may hold values from -0.1875 to 0.1875
- product_scale_vector: float32 [256], replicated, may hold values from 0.1 to 1.9
- twin_operand_matrix: bfloat16 [256, 64], replicated, may hold values from -0.375 to 0.375
- couple_projection_matrix: bfloat16 [1024, 128], replicated, may hold values from -0.1875 to 0.1875
Outputs:
- alignment_start_adjoint: bfloat16 [64, 1024, 256], P(('col', 'sub'), ('groups', 'row')), parts along dimension 1
- grad_out_weight: float32 [2048, 128], P('groups'), parts along dimension 0
- grad_factor_weight: float32 [512, 64], P('groups'), parts along dimension 0
- grad_w_in: float32 [512, 1024], P('groups'), parts along dimension 0
- grad_w_mid: float32 [2048, 256], P('groups'), parts along dimension 0
- feedforward_scale_adjoint: float32 [512], P('groups'), parts along dimension 0
- product_scale_adjoint: float32 [512], P('groups'), parts along dimension 0
The draws below stay inside these ranges and needn't reach their ends.
There are 2 independent parts, one for each index of `groups`. The reference program is written for one: setup_inputs(seed, part) draws one part's arguments, and reference() takes and returns one part's arrays. A program takes and returns all parts, laid end to end along the dimension named above; an argument that names none is the same for every part. Nothing has to cross between parts.
All inputs are finite; a program needn't handle non-finite values. No bound on the sum of `homolog_existence` or of `amino_existence` on one device may be relied on, other than what follows from the above.
Results may differ from the reference program's by a relative error of at most 0.015.
Values may be sent and summed in bfloat16 or wider, within the bound.
No kernel may reach another device: no remote copies, remote signals or barrier semaphores. Data moves between devices by JAX's collectives and lax.ppermute only.
A program may use at most 64 MiB of HBM per device.

```python
import math
import jax
import jax.numpy as jnp
from jax import lax

ALIGN_DIM = 256
HIDDEN_UNITS = 1024
PRODUCT_DIM = 32
P_SIZE = 128
HOMOLOG_TOTAL = 64
AMINO_SPAN = 512


def with_ends(values, own_key, low, largest):
    place = [jax.random.randint(jax.random.fold_in(own_key, axis), (), 0, length) for axis, length in enumerate(values.shape)]
    longest = values.shape.index(max(values.shape))
    neighbour = place[:longest] + [(place[longest] + 1) % values.shape[longest]] + place[longest + 1:]
    return values.at[tuple(place)].set(low).at[tuple(neighbour)].set(largest)


def levels(rng, dims, split, low, high):
    def one(dim, parts):
        steps = jax.random.uniform(jax.random.fold_in(jax.random.fold_in(rng, 6), dim), (parts,), jnp.float32, low / len(split), high / len(split))
        return jnp.repeat(jnp.exp(steps), dims[dim] // parts).reshape((-1,) + (1,) * (len(dims) - dim - 1))

    gain = one(*split[0])
    for cut in split[1:]:
        gain = gain * one(*cut)
    return gain


def bell_draw(key, extent, deviation, reach, pieces=(), kind=jnp.bfloat16):
    entries = deviation * jax.random.normal(key, extent, jnp.float32)
    if pieces:
        entries = entries * levels(key, extent, pieces, -0.22, 0.18)
    return jnp.clip(entries, -reach, reach).astype(kind)


def setup_inputs(seed: int = 0, part: int = 0) -> dict:
    seeds = jax.random.split(jax.random.key(seed), 12)
    part_keys = jax.random.split(jax.random.fold_in(seeds[11], part), 12)
    saved_alignment = bell_draw(part_keys[0], (HOMOLOG_TOTAL, AMINO_SPAN, ALIGN_DIM), 1.0, 6.0, ((0, 8), (1, 16)))
    homolog_existence = with_ends((jax.random.randint(part_keys[1], (HOMOLOG_TOTAL, AMINO_SPAN), 0, 8) < 7).astype(jnp.int32), jax.random.fold_in(part_keys[1], 1), 0, 1)
    amino_existence = with_ends((jax.random.randint(part_keys[2], (AMINO_SPAN,), 0, 8) < 7).astype(jnp.int32), jax.random.fold_in(part_keys[2], 1), 0, 1)
    couple_delta_adjoint = bell_draw(part_keys[3], (AMINO_SPAN, AMINO_SPAN, P_SIZE), 0.25, 1.5, ((0, 16), (1, 8)))
    feedforward_adjoint = bell_draw(part_keys[4], (HOMOLOG_TOTAL, AMINO_SPAN, ALIGN_DIM), 0.25, 1.5, ((0, 8), (1, 16)))
    feedforward_scale = jnp.clip(1.0 + 0.18 * jax.random.normal(seeds[5], (ALIGN_DIM,), jnp.float32), 0.1, 1.9)
    expansion_matrix = bell_draw(seeds[6], (ALIGN_DIM, HIDDEN_UNITS), ALIGN_DIM ** -0.5, 0.375)
    contraction_matrix = bell_draw(seeds[7], (HIDDEN_UNITS, ALIGN_DIM), HIDDEN_UNITS ** -0.5, 0.1875)
    product_scale_vector = jnp.clip(1.0 + 0.18 * jax.random.normal(seeds[8], (ALIGN_DIM,), jnp.float32), 0.1, 1.9)
    twin_operand_matrix = bell_draw(seeds[9], (ALIGN_DIM, 2 * PRODUCT_DIM), ALIGN_DIM ** -0.5, 0.375)
    couple_projection_matrix = bell_draw(seeds[10], (PRODUCT_DIM * PRODUCT_DIM, P_SIZE), (PRODUCT_DIM * PRODUCT_DIM) ** -0.5, 0.1875)
    return dict(saved_alignment=saved_alignment, homolog_existence=homolog_existence, amino_existence=amino_existence, couple_delta_adjoint=couple_delta_adjoint, feedforward_adjoint=feedforward_adjoint, feedforward_scale=feedforward_scale, expansion_matrix=expansion_matrix, contraction_matrix=contraction_matrix, product_scale_vector=product_scale_vector, twin_operand_matrix=twin_operand_matrix, couple_projection_matrix=couple_projection_matrix)


epsilon = 1e-05

def layer_normalize(values):
    centre = lax.optimization_barrier(jnp.mean(values, axis=-1, keepdims=True))
    centred = values - centre
    variance = lax.optimization_barrier(jnp.mean(centred * centred, axis=-1, keepdims=True))
    inv_std = lax.rsqrt(variance + epsilon)
    return (centred * inv_std, inv_std)

def standardizer_adjoint(grad_hat, normed, inv_std):
    first_mean = lax.optimization_barrier(jnp.mean(grad_hat, axis=-1, keepdims=True))
    second_mean = lax.optimization_barrier(jnp.mean(grad_hat * normed, axis=-1, keepdims=True))
    return inv_std * (grad_hat - first_mean - normed * second_mean)

def exact_gelu(values):
    return jax.nn.gelu(values, approximate=False)

def reference(saved_alignment, homolog_existence, amino_existence, couple_delta_adjoint, feedforward_adjoint, feedforward_scale, expansion_matrix, contraction_matrix, product_scale_vector, twin_operand_matrix, couple_projection_matrix):
    existing_record_lines = HOMOLOG_TOTAL * AMINO_SPAN
    embedding_numbers = saved_alignment.astype(jnp.float32).reshape(existing_record_lines, ALIGN_DIM)
    transition_standardized, transition_inv_deviation = layer_normalize(embedding_numbers)
    normalized_input = (transition_standardized * feedforward_scale).astype(jnp.bfloat16)
    hidden_pre = jnp.dot(normalized_input, expansion_matrix, preferred_element_type=jnp.float32)
    gelu_value, gelu_back = jax.vjp(exact_gelu, hidden_pre)
    hidden = gelu_value.astype(jnp.bfloat16)
    mixed_values = embedding_numbers + jnp.dot(hidden, contraction_matrix, preferred_element_type=jnp.float32)
    product_zscored, product_reciprocal_spread = layer_normalize(mixed_values)
    normalized_output = (product_zscored * product_scale_vector).astype(jnp.bfloat16)
    projected = jnp.dot(normalized_output, twin_operand_matrix, preferred_element_type=jnp.float32)
    keep_mask = (homolog_existence * amino_existence[None, :]).astype(jnp.float32)
    keep_col = keep_mask.reshape(existing_record_lines, 1)
    left_factor = (projected[:, :PRODUCT_DIM] * keep_col).astype(jnp.bfloat16).reshape(HOMOLOG_TOTAL, AMINO_SPAN, PRODUCT_DIM)
    right_factor = (projected[:, PRODUCT_DIM:] * keep_col).astype(jnp.bfloat16).reshape(HOMOLOG_TOTAL, AMINO_SPAN, PRODUCT_DIM)
    pair_count = jnp.dot(keep_mask.T, keep_mask, precision=lax.Precision.HIGHEST)
    inverse = 1.0 / jnp.maximum(pair_count, 1.0)
    block_rows = math.gcd(AMINO_SPAN, 16)
    block_total = AMINO_SPAN // block_rows
    left_wide = left_factor.astype(jnp.float32)
    right_wide = right_factor.astype(jnp.float32)
    out_wide = couple_projection_matrix.astype(jnp.float32)

    def block_step(running, block_index):
        result_adjoint, grad_right = running
        row_start = block_index * block_rows
        left_block = lax.dynamic_slice_in_dim(left_wide, row_start, block_rows, 1)
        inv_block = lax.dynamic_slice_in_dim(inverse, row_start, block_rows, 0)
        cot_block = lax.dynamic_slice_in_dim(couple_delta_adjoint, row_start, block_rows, 0).astype(jnp.float32)
        outer_sum = jnp.einsum('sip,sjq->ijpq', left_block, right_wide)
        outer_half = lax.optimization_barrier((outer_sum * inv_block[:, :, None, None]).astype(jnp.bfloat16))
        outer_flat = outer_half.astype(jnp.float32).reshape(block_rows, AMINO_SPAN, PRODUCT_DIM * PRODUCT_DIM)
        result_adjoint = result_adjoint + jnp.einsum('ijk,ijl->kl', outer_flat, cot_block)
        pair_back = jnp.einsum('ijl,kl->ijk', cot_block, out_wide) * inv_block[:, :, None]
        back_half = lax.optimization_barrier(pair_back.astype(jnp.bfloat16))
        back_wide = back_half.astype(jnp.float32).reshape(block_rows, AMINO_SPAN, PRODUCT_DIM, PRODUCT_DIM)
        grad_left_block = jnp.einsum('ijpq,sjq->sip', back_wide, right_wide)
        grad_right = grad_right + jnp.einsum('ijpq,sip->sjq', back_wide, left_block)
        return ((result_adjoint, grad_right), grad_left_block)
    start_state = (jnp.zeros((PRODUCT_DIM * PRODUCT_DIM, P_SIZE), jnp.float32), jnp.zeros((HOMOLOG_TOTAL, AMINO_SPAN, PRODUCT_DIM), jnp.float32))
    (result_adjoint, grad_right), left_blocks = lax.scan(block_step, start_state, jnp.arange(block_total, dtype=jnp.int32))
    grad_left = jnp.transpose(left_blocks, (1, 0, 2, 3)).reshape(HOMOLOG_TOTAL, AMINO_SPAN, PRODUCT_DIM)
    grad_proj = jnp.concatenate([grad_left.reshape(existing_record_lines, PRODUCT_DIM), grad_right.reshape(existing_record_lines, PRODUCT_DIM)], axis=1)
    grad_proj = (grad_proj * keep_col).astype(jnp.bfloat16)
    operand_adjoint = jnp.dot(normalized_output.T, grad_proj, preferred_element_type=jnp.float32)
    rescaled_result_adjoint = jnp.dot(grad_proj, twin_operand_matrix.T, preferred_element_type=jnp.float32)
    product_scale_adjoint = lax.optimization_barrier(jnp.sum(rescaled_result_adjoint * product_zscored, axis=0))
    combined_adjoint = feedforward_adjoint.astype(jnp.float32).reshape(existing_record_lines, ALIGN_DIM) + standardizer_adjoint(rescaled_result_adjoint * product_scale_vector, product_zscored, product_reciprocal_spread)
    grad_mixed_half = combined_adjoint.astype(jnp.bfloat16)
    hidden_adjoint = jnp.dot(hidden.T, grad_mixed_half, preferred_element_type=jnp.float32)
    grad_hidden = jnp.dot(grad_mixed_half, contraction_matrix.T, preferred_element_type=jnp.float32)
    grad_pre = gelu_back(grad_hidden)[0].astype(jnp.bfloat16)
    expansion_adjoint = jnp.dot(normalized_input.T, grad_pre, preferred_element_type=jnp.float32)
    normed_input_gradient = jnp.dot(grad_pre, expansion_matrix.T, preferred_element_type=jnp.float32)
    feedforward_scale_adjoint = lax.optimization_barrier(jnp.sum(normed_input_gradient * transition_standardized, axis=0))
    alignment_start_adjoint = combined_adjoint + standardizer_adjoint(normed_input_gradient * feedforward_scale, transition_standardized, transition_inv_deviation)
    return (alignment_start_adjoint.astype(jnp.bfloat16).reshape(HOMOLOG_TOTAL, AMINO_SPAN, ALIGN_DIM), result_adjoint, operand_adjoint, expansion_adjoint, hidden_adjoint, feedforward_scale_adjoint, product_scale_adjoint)
```

```python
import math

import jax
import jax.numpy as jnp
from jax import lax
from jax.sharding import PartitionSpec as P

epsilon = 1e-05


lanes = 128


def spread(own, axis):
    everyone = jnp.broadcast_to(own, (lax.axis_size(axis),) + own.shape)
    return lax.all_to_all(everyone, axis, split_axis=0, concat_axis=0, tiled=True)


def reduced(parts, axis):
    arrived = lax.all_to_all(parts, axis, split_axis=0, concat_axis=0, tiled=True)
    return arrived.astype(jnp.float32).sum(axis=0).astype(jnp.bfloat16)


def cut(array):
    return jnp.moveaxis(array.reshape(array.shape[0], -1, lanes), 1, 0).reshape(-1, lanes)


def uncut(lines, shape):
    return jnp.moveaxis(lines.reshape(-1, shape[0], lanes), 0, 1).reshape(shape)


def summed_everywhere(grads):
    cols, rows = lax.axis_size("col"), lax.axis_size("row")
    whole = [g.ndim == 2 and g.shape[-1] % lanes == 0 for g in grads]
    pieces = [cut(g) if w else g.reshape(-1, lanes) for g, w in zip(grads, whole)]
    lines = jnp.concatenate([p.astype(jnp.bfloat16) for p in pieces], axis=0)
    lines = jnp.pad(lines, ((0, -lines.shape[0] % (2 * cols * rows * 8)), (0, 0)))
    halves = lines.reshape(2, lines.shape[0] // 2, lanes)
    mine = lax.axis_index("sub")
    swap = [(0, 1), (1, 0)]
    kept = lax.dynamic_index_in_dim(halves, mine, 0, keepdims=False)
    sent = lax.dynamic_index_in_dim(halves, 1 - mine, 0, keepdims=False)
    half = kept.astype(jnp.float32) + lax.ppermute(sent, "sub", swap).astype(jnp.float32)
    part = reduced(half.astype(jnp.bfloat16).reshape(cols, -1, lanes), "col")
    part = reduced(part.reshape(rows, -1, lanes), "row")
    part = spread(part, "row").reshape(-1, lanes)
    half = spread(part, "col").reshape(-1, lanes)
    other = lax.ppermute(half, "sub", swap)
    first = jnp.where(mine == 0, half, other)
    second = jnp.where(mine == 0, other, half)
    lines = jnp.concatenate([first, second], axis=0)
    done, at = [], 0
    for g, p, w in zip(grads, pieces, whole):
        own = lines[at : at + p.shape[0]].astype(jnp.float32)
        at += p.shape[0]
        done.append(uncut(own, g.shape) if w else own.reshape(g.shape))
    return tuple(done)


def layer_normalize(values):
    centre = jnp.mean(values, axis=-1, keepdims=True)
    centred = values - centre
    variance = jnp.mean(centred * centred, axis=-1, keepdims=True)
    inv_std = lax.rsqrt(variance + epsilon)
    return (centred * inv_std, inv_std)


def standardizer_adjoint(grad_hat, normed, inv_std):
    first_mean = jnp.mean(grad_hat, axis=-1, keepdims=True)
    second_mean = jnp.mean(grad_hat * normed, axis=-1, keepdims=True)
    return inv_std * (grad_hat - first_mean - normed * second_mean)


def exact_gelu(values):
    return jax.nn.gelu(values, approximate=False)


def contract_rows(first_arr, second_arr):
    return lax.dot_general(
        first_arr, second_arr, (((0,), (0,)), ((), ())), preferred_element_type=jnp.float32
    )


def contract_last(first_arr, second_arr):
    return lax.dot_general(
        first_arr, second_arr, (((1,), (1,)), ((), ())), preferred_element_type=jnp.float32
    )


def per_device(
    saved_alignment,
    homolog_existence,
    amino_existence,
    couple_delta_adjoint,
    feedforward_adjoint,
    feedforward_scale,
    expansion_matrix,
    contraction_matrix,
    product_scale_vector,
    twin_operand_matrix,
    couple_projection_matrix,
):
    homolog_split_total, amino_split_total, lane_breadth = saved_alignment.shape
    factor = twin_operand_matrix.shape[1] // 2
    pair_width = couple_projection_matrix.shape[1]
    existing_record_lines = homolog_split_total * amino_split_total
    shard_count = lax.axis_size(("col", "sub"))
    row_devices = lax.axis_size("row")
    total_res = amino_split_total * row_devices
    col_res = total_res // shard_count
    all_seqs = homolog_split_total * shard_count
    embedding_numbers = saved_alignment.astype(jnp.float32).reshape(
        existing_record_lines, lane_breadth
    )
    transition_standardized, transition_inv_deviation = layer_normalize(embedding_numbers)
    normalized_input = (transition_standardized * feedforward_scale).astype(jnp.bfloat16)
    hidden_pre = jnp.dot(normalized_input, expansion_matrix, preferred_element_type=jnp.float32)
    gelu_value, gelu_back = jax.vjp(exact_gelu, hidden_pre)
    hidden = gelu_value.astype(jnp.bfloat16)
    mixed_values = embedding_numbers + jnp.dot(
        hidden, contraction_matrix, preferred_element_type=jnp.float32
    )
    product_zscored, product_reciprocal_spread = layer_normalize(mixed_values)
    normalized_output = (product_zscored * product_scale_vector).astype(jnp.bfloat16)
    projected = jnp.dot(normalized_output, twin_operand_matrix, preferred_element_type=jnp.float32)
    keep_mask = (homolog_existence * amino_existence[None, :]).astype(jnp.float32)
    keep_col = keep_mask.reshape(existing_record_lines, 1)
    left_factor = (
        (projected[:, :factor] * keep_col)
        .astype(jnp.bfloat16)
        .reshape(homolog_split_total, amino_split_total * factor)
    )
    right_factor = (
        (projected[:, factor:] * keep_col)
        .astype(jnp.bfloat16)
        .reshape(homolog_split_total, amino_split_total * factor)
    )
    wide = amino_split_total * factor
    blocks = row_devices // shard_count
    keep_half = jnp.pad(
        keep_mask.astype(jnp.bfloat16), ((0, 0), (0, -amino_split_total % lanes))
    )
    right_record = jnp.concatenate([right_factor, keep_half], axis=1)
    left_record = jnp.concatenate([left_factor, keep_half], axis=1)
    right_spread = spread(right_record, "row").reshape(
        shard_count, blocks, homolog_split_total, right_record.shape[1]
    )
    left_spread = jnp.broadcast_to(left_record, (shard_count, 1) + left_record.shape)
    records = lax.all_to_all(
        jnp.concatenate([right_spread, left_spread], axis=1),
        ("col", "sub"),
        split_axis=0,
        concat_axis=0,
        tiled=True,
    )
    right_records = jnp.moveaxis(records[:, :blocks], 1, 2).reshape(all_seqs, blocks, -1)
    left_records = records[:, blocks].reshape(all_seqs, -1)
    right_cols = right_records[:, :, :wide].reshape(all_seqs, col_res, factor)
    left_rows = left_records[:, :wide].reshape(all_seqs, amino_split_total, factor)
    keep_cols = right_records[:, :, wide : wide + amino_split_total].reshape(all_seqs, col_res)
    keep_rows = left_records[:, wide : wide + amino_split_total]
    pair_count = contract_rows(keep_rows, keep_cols)
    inverse = 1.0 / jnp.maximum(pair_count, 1.0)
    block_rows = math.gcd(amino_split_total, 16)
    result_adjoint = jnp.zeros((factor * factor, pair_width), jnp.float32)
    grad_right = jnp.zeros((all_seqs, col_res, factor), jnp.float32)
    left_parts = []
    for row_start in range(0, amino_split_total, block_rows):
        left_block = left_rows[:, row_start : row_start + block_rows, :]
        inv_block = inverse[row_start : row_start + block_rows]
        cot_block = couple_delta_adjoint[row_start : row_start + block_rows]
        outer_sum = jnp.einsum(
            "sip,sjq->ijpq", left_block, right_cols, preferred_element_type=jnp.float32
        )
        outer_half = (outer_sum * inv_block[:, :, None, None]).astype(jnp.bfloat16)
        outer_half = outer_half.reshape(block_rows, col_res, factor * factor)
        result_adjoint = result_adjoint + jnp.einsum(
            "ijk,ijl->kl", outer_half, cot_block, preferred_element_type=jnp.float32
        )
        pair_back = jnp.einsum(
            "ijl,kl->ijk", cot_block, couple_projection_matrix, preferred_element_type=jnp.float32
        )
        back_half = (pair_back * inv_block[:, :, None]).astype(jnp.bfloat16)
        back_half = back_half.reshape(block_rows, col_res, factor, factor)
        left_parts.append(
            jnp.einsum("ijpq,sjq->sip", back_half, right_cols, preferred_element_type=jnp.float32)
        )
        grad_right = grad_right + jnp.einsum(
            "ijpq,sip->sjq", back_half, left_block, preferred_element_type=jnp.float32
        )
    grad_left = jnp.concatenate(left_parts, axis=1).reshape(all_seqs, amino_split_total * factor)
    back = jnp.concatenate(
        [
            jnp.moveaxis(
                grad_right.astype(jnp.bfloat16).reshape(
                    shard_count, homolog_split_total, blocks, wide
                ),
                2,
                1,
            ),
            grad_left.astype(jnp.bfloat16).reshape(shard_count, 1, homolog_split_total, wide),
        ],
        axis=1,
    )
    back = lax.all_to_all(back, ("col", "sub"), split_axis=0, concat_axis=0, tiled=True)
    left_own = back[:, blocks].astype(jnp.float32).sum(axis=0)
    right_back = back[:, :blocks].reshape(row_devices, homolog_split_total, wide)
    right_back = lax.all_to_all(right_back, "row", split_axis=0, concat_axis=0, tiled=True)
    right_own = right_back.astype(jnp.float32).sum(axis=0)
    grad_proj = jnp.concatenate(
        [
            left_own.reshape(existing_record_lines, factor),
            right_own.reshape(existing_record_lines, factor),
        ],
        axis=1,
    )
    grad_proj = (grad_proj * keep_col).astype(jnp.bfloat16)
    operand_adjoint = contract_rows(normalized_output, grad_proj)
    rescaled_result_adjoint = contract_last(grad_proj, twin_operand_matrix)
    product_scale_adjoint = jnp.sum(rescaled_result_adjoint * product_zscored, axis=0)
    combined_adjoint = feedforward_adjoint.astype(jnp.float32).reshape(
        existing_record_lines, lane_breadth
    ) + standardizer_adjoint(
        rescaled_result_adjoint * product_scale_vector, product_zscored, product_reciprocal_spread
    )
    grad_mixed_half = combined_adjoint.astype(jnp.bfloat16)
    hidden_adjoint = contract_rows(hidden, grad_mixed_half)
    grad_hidden = contract_last(grad_mixed_half, contraction_matrix)
    grad_pre = gelu_back(grad_hidden)[0].astype(jnp.bfloat16)
    expansion_adjoint = contract_rows(normalized_input, grad_pre)
    normed_input_gradient = contract_last(grad_pre, expansion_matrix)
    feedforward_scale_adjoint = jnp.sum(normed_input_gradient * transition_standardized, axis=0)
    alignment_start_adjoint = combined_adjoint + standardizer_adjoint(
        normed_input_gradient * feedforward_scale, transition_standardized, transition_inv_deviation
    )
    weight_grads = summed_everywhere(
        (
            result_adjoint,
            operand_adjoint,
            expansion_adjoint,
            hidden_adjoint,
            feedforward_scale_adjoint,
            product_scale_adjoint,
        )
    )
    return (
        alignment_start_adjoint.astype(jnp.bfloat16).reshape(
            homolog_split_total, amino_split_total, lane_breadth
        ),
        weight_grads[0],
        weight_grads[1],
        weight_grads[2],
        weight_grads[3],
        weight_grads[4],
        weight_grads[5],
    )


def solution(mesh):
    return jax.shard_map(
        per_device,
        mesh=mesh,
        in_specs=(
            P(("col", "sub"), ("groups", "row"), None),
            P(("col", "sub"), ("groups", "row")),
            P(("groups", "row")),
            P(("groups", "row"), ("col", "sub"), None),
            P(("col", "sub"), ("groups", "row"), None),
            P(),
            P(),
            P(),
            P(),
            P(),
            P(),
        ),
        out_specs=(
            P(("col", "sub"), ("groups", "row"), None),
            P("groups", None),
            P("groups", None),
            P("groups", None),
            P("groups", None),
            P("groups"),
            P("groups"),
        ),
        check_vma=False,
    )
```

```python
import math

import jax
import jax.numpy as jnp
from jax import lax
from jax.experimental import pallas as pl
from jax.experimental.pallas import tpu as pltpu
from jax.sharding import PartitionSpec as P

epsilon = 1e-05
lanes = 128
f32 = jnp.float32
bf16 = jnp.bfloat16
INTERPRET = False


def layer_normalize(values):
    centre = jnp.mean(values, axis=-1, keepdims=True)
    centred = values - centre
    variance = jnp.mean(centred * centred, axis=-1, keepdims=True)
    inv_std = lax.rsqrt(variance + epsilon)
    return (centred * inv_std, inv_std)


def standardizer_adjoint(grad_hat, normed, inv_std):
    first_mean = jnp.mean(grad_hat, axis=-1, keepdims=True)
    second_mean = jnp.mean(grad_hat * normed, axis=-1, keepdims=True)
    return inv_std * (grad_hat - first_mean - normed * second_mean)


def plain(a, b):
    return lax.dot_general(a, b, (((1,), (0,)), ((), ())), preferred_element_type=f32)


def last_last(a, b):
    return lax.dot_general(a, b, (((1,), (1,)), ((), ())), preferred_element_type=f32)


def first_first(a, b):
    return lax.dot_general(a, b, (((0,), (0,)), ((), ())), preferred_element_type=f32)


def turn(values, shift):
    shift = shift % lanes
    return values if shift == 0 else pltpu.roll(values, shift, 1)


def lane_index(shape):
    return lax.broadcasted_iota(jnp.int32, shape, 1)


def keep_column(keep, seqs, res):
    rows = seqs * res
    wide = jnp.broadcast_to(keep[:, None, :], (seqs, res, lanes)).reshape(rows, lanes)
    residue = lax.broadcasted_iota(jnp.int32, (rows, lanes), 0) % res
    own = lane_index((rows, lanes)) == residue
    return jnp.sum(jnp.where(own, wide, 0.0), axis=1, keepdims=True)


def forward_kernel(
    x_ref, keep_ref, scale_in_ref, w_in_ref, w_mid_ref, scale_out_ref, twin_ref,
    right_ref, left_ref, normed_in_ref, hidden_ref, slope_ref, hat_in_ref, hat_out_ref,
    normed_out_ref, spread_ref, left_rows, right_rows,
):
    seqs = keep_ref.shape[0]
    rows = x_ref.shape[0]
    res = rows // seqs
    factor = twin_ref.shape[0] // 2
    group = lanes // factor
    x = x_ref[...].astype(f32)
    hat_in, inv_in = layer_normalize(x)
    hat_in_ref[...] = hat_in
    normed_in = (hat_in * scale_in_ref[...]).astype(bf16)
    normed_in_ref[...] = normed_in
    pre = plain(normed_in, w_in_ref[...])
    share = 0.5 * (1.0 + lax.erf(pre * math.sqrt(0.5)))
    hidden = (pre * share).astype(bf16)
    hidden_ref[...] = hidden
    slope_ref[...] = share + pre * (jnp.exp(-0.5 * pre * pre) * (1.0 / math.sqrt(2.0 * math.pi)))
    mixed = x + plain(hidden, w_mid_ref[...])
    hat_out, inv_out = layer_normalize(mixed)
    hat_out_ref[...] = hat_out
    lane = lane_index((rows, lanes))
    spread_ref[...] = jnp.where(lane == 0, inv_in, inv_out)
    normed_out = (hat_out * scale_out_ref[...]).astype(bf16)
    normed_out_ref[...] = normed_out
    keep = keep_ref[...]
    twin = twin_ref[...]
    projected = last_last(
        normed_out, jnp.concatenate([twin, jnp.zeros((lanes - 2 * factor, twin.shape[1]), bf16)], axis=0)
    )
    left_rows[...] = jnp.where(lane < factor, projected * keep_column(keep, seqs, res), 0.0)
    turned = last_last(twin[factor:], normed_out)
    per = lanes // res
    for s in range(seqs):
        tile = turned[:, (s // per) * lanes : (s // per + 1) * lanes]
        right_rows[s * factor : (s + 1) * factor, :] = turn(tile, -(s % per) * res)
    for t in range(res // group):
        tile = left_rows[pl.ds(t * group, seqs, stride=res), :]
        for m in range(1, group):
            tile = tile + turn(left_rows[pl.ds(t * group + m, seqs, stride=res), :], m * factor)
        left_ref[:, t * lanes : (t + 1) * lanes] = tile.astype(bf16)
    left_ref[:, res * factor :] = keep.astype(bf16)
    pieces = []
    for t in range(factor // per):
        tile = right_rows[pl.ds(t * per, seqs, stride=factor), :] * keep
        for m in range(1, per):
            piece = right_rows[pl.ds(t * per + m, seqs, stride=factor), :] * keep
            tile = tile + turn(piece, m * res)
        pieces.append(tile)
    record = jnp.concatenate(pieces + [keep], axis=1).astype(bf16)
    for c in range(right_ref.shape[0]):
        right_ref[c] = record


def pair_kernel(
    rec_ref, cot_ref, proj_ref, back_ref, grad_ref,
    left_all, right_all, outer_all, adjoint_all, pulled_all, proj_rows, proj_all,
):
    shards, parts, seqs, _ = rec_ref.shape
    blocks = parts - 1
    all_seqs = shards * seqs
    res = cot_ref.shape[0]
    cols = cot_ref.shape[1]
    wide = back_ref.shape[3]
    factor = wide // res
    pairs = lanes // cols
    sets = factor // pairs
    half = cols // blocks
    lane = lane_index((all_seqs, lanes))

    def gathered(part, t):
        return rec_ref[:, part, :, t * lanes : (t + 1) * lanes].astype(f32).reshape(all_seqs, lanes)

    for t in range(wide // lanes):
        left_all[:, t * lanes : (t + 1) * lanes] = gathered(blocks, t).astype(bf16)
        a, b = gathered(0, t), gathered(1, t)
        first = jnp.where(
            lane < 32, a, jnp.where(lane < 64, turn(b, 32), jnp.where(lane < 96, turn(a, 32), turn(b, 64)))
        )
        second = jnp.where(
            lane < 32, turn(a, 64), jnp.where(lane < 64, turn(b, 96), jnp.where(lane < 96, turn(a, 96), b))
        )
        right_all[:, 2 * t * lanes : (2 * t + 1) * lanes] = first.astype(bf16)
        right_all[:, (2 * t + 1) * lanes : (2 * t + 2) * lanes] = second.astype(bf16)
    last = wide // lanes
    keep_rows = gathered(blocks, last).astype(bf16)
    keep_cols = (gathered(0, last) + turn(gathered(1, last), half)).astype(bf16)
    count = first_first(keep_cols, keep_rows)[:cols]
    inverse = 1.0 / jnp.maximum(count, 1.0)
    nothing = jnp.zeros((cols, lanes), bf16)
    for i in range(res):
        scaled = (cot_ref[i].astype(f32) * inverse[:, i : i + 1]).astype(bf16)
        at = i * lanes
        for k in range(pairs):
            for m in range(pairs):
                adjoint_all[at + k * cols : at + (k + 1) * cols, m * lanes : (m + 1) * lanes] = (
                    scaled if k == m else nothing
                )
    proj_rows[...] = proj_ref[...].astype(f32)
    for n in range(sets):
        for k in range(pairs):
            proj_all[n * factor : (n + 1) * factor, k * lanes : (k + 1) * lanes] = proj_rows[
                pl.ds(n * pairs + k, factor, stride=factor), :
            ].astype(bf16)
    step = 256 // factor
    for c in range(res // step):
        outer = first_first(left_all[:, c * step * factor : (c + 1) * step * factor], right_all[...])
        for i in range(step):
            at = (c * step + i) * lanes
            for n in range(sets):
                outer_all[n * factor : (n + 1) * factor, at : at + lanes] = outer[
                    i * factor : (i + 1) * factor, n * lanes : (n + 1) * lanes
                ].astype(bf16)
        pulled = last_last(proj_all[...], adjoint_all[c * step * lanes : (c + 1) * step * lanes, :])
        for i in range(step):
            at = (c * step + i) * factor
            for n in range(sets):
                pulled_all[at : at + factor, n * lanes : (n + 1) * lanes] = pulled[
                    n * factor : (n + 1) * factor, i * lanes : (i + 1) * lanes
                ].astype(bf16)
    grad_ref[...] = plain(outer_all[...], adjoint_all[...])
    grad_left = last_last(right_all[...], pulled_all[...])
    grad_right = plain(left_all[...], pulled_all[...])

    def put(part, t, values):
        back_ref[:, part, :, t * lanes : (t + 1) * lanes] = values.reshape(shards, seqs, lanes).astype(bf16)

    for t in range(wide // lanes):
        put(blocks, t, grad_left[:, t * lanes : (t + 1) * lanes])
        a = grad_right[:, 2 * t * lanes : (2 * t + 1) * lanes]
        b = grad_right[:, (2 * t + 1) * lanes : (2 * t + 2) * lanes]
        put(0, t, jnp.where(
            lane < 32, a, jnp.where(lane < 64, turn(a, 96), jnp.where(lane < 96, turn(b, 64), turn(b, 32)))
        ))
        put(1, t, jnp.where(
            lane < 32, turn(a, 96), jnp.where(lane < 64, turn(a, 64), jnp.where(lane < 96, turn(b, 32), b))
        ))


def chunk_rows(rows, features, hidden, factor, pair_width, chunks):
    sizes = (
        features * hidden // chunks // lanes,
        hidden * features // chunks // lanes,
        factor * factor * pair_width // chunks // lanes,
        2 * factor * features // chunks // lanes,
    )
    starts = [0]
    for size in sizes:
        starts.append(starts[-1] + size)
    return starts


def backward_kernel(
    core_ref, left_ref, right_ref, keep_ref, cot_ref, scale_in_ref, w_in_ref, w_mid_ref, scale_out_ref,
    twin_ref, grad_ref, normed_in_ref, hidden_ref, slope_ref, hat_in_ref, hat_out_ref, normed_out_ref,
    spread_ref, out_ref, own_ref, send_ref, left_rows, right_rows, chunks_ref,
):
    seqs = keep_ref.shape[0]
    rows, features = cot_ref.shape
    res = rows // seqs
    factor = twin_ref.shape[0] // 2
    group = lanes // factor
    per = lanes // res
    cols = own_ref.shape[0]
    chunks = 2 * cols
    units = hidden_ref.shape[1]
    pair_width = lanes
    starts = chunk_rows(rows, features, units, factor, pair_width, chunks)
    keep = keep_ref[...]
    lane_small = lane_index((seqs, lanes))
    last = left_ref.shape[1] - 1
    for t in range(res // group):
        tile = jnp.sum(left_ref[:, last, :, t * lanes : (t + 1) * lanes].astype(f32), axis=0)
        for m in range(group):
            piece = jnp.where(lane_small < factor, turn(tile, -m * factor), 0.0)
            left_rows[pl.ds(t * group + m, seqs, stride=res), :] = piece
    for t in range(factor // per):
        tile = jnp.sum(right_ref[:, :, t * lanes : (t + 1) * lanes].astype(f32), axis=0)
        for m in range(per):
            right_rows[pl.ds(t * per + m, seqs, stride=factor), :] = turn(tile, -m * res) * keep
    tiles = []
    for h in range(rows // lanes):
        tile = right_rows[h * per * factor : (h * per + 1) * factor, :]
        for m in range(1, per):
            at = (h * per + m) * factor
            tile = tile + turn(right_rows[at : at + factor, :], m * res)
        tiles.append(tile)
    turned = jnp.concatenate(tiles, axis=1)
    turned = jnp.concatenate(
        [jnp.zeros((factor, rows), f32), turned, jnp.zeros((lanes - 2 * factor, rows), f32)], axis=0
    )
    grad_proj = (left_rows[...] * keep_column(keep, seqs, res) + jnp.transpose(turned)).astype(bf16)
    twin = twin_ref[...]
    twin = jnp.concatenate([twin, jnp.zeros((lanes - 2 * factor, features), bf16)], axis=0)
    operand_adjoint = first_first(grad_proj, normed_out_ref[...])
    rescaled = plain(grad_proj, twin)
    hat_out = hat_out_ref[...]
    product_adjoint = jnp.sum(rescaled * hat_out, axis=0, keepdims=True)
    inv_in = spread_ref[:, 0:1]
    inv_out = spread_ref[:, 1:2]
    combined = cot_ref[...].astype(f32) + standardizer_adjoint(
        rescaled * scale_out_ref[...], hat_out, inv_out
    )
    mixed_half = combined.astype(bf16)
    grad_hidden = last_last(mixed_half, w_mid_ref[...])
    grad_pre = (slope_ref[...] * grad_hidden).astype(bf16)
    grad_in = last_last(grad_pre, w_in_ref[...])
    hat_in = hat_in_ref[...]
    scale_adjoint = jnp.sum(grad_in * hat_in, axis=0, keepdims=True)
    out_ref[...] = (
        combined + standardizer_adjoint(grad_in * scale_in_ref[...], hat_in, inv_in)
    ).astype(bf16)
    hidden_adjoint = first_first(hidden_ref[...], mixed_half)
    expansion_adjoint = first_first(normed_in_ref[...], grad_pre)
    split = features // lanes

    def put(k, at, values):
        chunks_ref[k // cols, k % cols, at : at + values.shape[0], :] = values.astype(bf16)

    unit_step = units // chunks
    for k in range(chunks):
        put(k, starts[0], expansion_adjoint[:, k * unit_step : (k + 1) * unit_step])
        for m in range(split):
            put(k, starts[1] + m * unit_step,
                hidden_adjoint[k * unit_step : (k + 1) * unit_step, m * lanes : (m + 1) * lanes])
        height = grad_ref.shape[0] // chunks
        for m in range(grad_ref.shape[1] // lanes):
            put(k, starts[2] + m * height, grad_ref[k * height : (k + 1) * height, m * lanes : (m + 1) * lanes])
        height = 2 * factor // chunks
        tail = [
            operand_adjoint[k * height : (k + 1) * height, m * lanes : (m + 1) * lanes] for m in range(split)
        ]
        row = lax.broadcasted_iota(jnp.int32, (8, lanes), 0)
        extra = jnp.zeros((8, lanes), f32)
        if k == 0:
            for n, vector in enumerate((scale_adjoint, product_adjoint)):
                for m in range(split):
                    extra = jnp.where(row == n * split + m, vector[:, m * lanes : (m + 1) * lanes], extra)
        rest = chunks_ref.shape[2] - starts[4] - 8
        block = jnp.concatenate(tail + [extra, jnp.zeros((rest, lanes), f32)], axis=0)
        put(k, starts[3], block)
    core = core_ref[0]
    own_ref[...] = chunks_ref[core]
    send_ref[...] = chunks_ref[1 - core]


def final_kernel(
    core_ref, half_ref, other_ref, grad_ref, twin_ref, w_in_ref, w_mid_ref, scale_ref, product_ref
):
    cols = half_ref.shape[0]
    chunks = 2 * cols
    features, units = w_in_ref.shape
    factor = twin_ref.shape[0] // 2
    starts = chunk_rows(0, features, units, factor, lanes, chunks)
    split = features // lanes
    unit_step = units // chunks
    core = core_ref[0]
    height = factor * factor // 2 // chunks
    for k in range(chunks):
        mine = core == k // cols

        def read(at, size):
            return jnp.where(
                mine,
                half_ref[k % cols, at : at + size, :].astype(f32),
                other_ref[k % cols, at : at + size, :].astype(f32),
            )

        w_in_ref[:, k * unit_step : (k + 1) * unit_step] = read(starts[0], features)
        for m in range(split):
            w_mid_ref[k * unit_step : (k + 1) * unit_step, m * lanes : (m + 1) * lanes] = read(
                starts[1] + m * unit_step, unit_step
            )
        for m in range(2):
            block = read(starts[2] + m * height, height)
            for n in range(height // factor):
                q = 2 * (k * (height // factor) + n) + m
                grad_ref[pl.ds(q, factor, stride=factor), :] = block[n * factor : (n + 1) * factor]
        tall = 2 * factor // chunks
        block = read(starts[3], starts[4] - starts[3])
        for m in range(split):
            twin_ref[k * tall : (k + 1) * tall, m * lanes : (m + 1) * lanes] = block[m * tall : (m + 1) * tall]
        if k == 0:
            extra = read(starts[4], 8)
            for n, ref in enumerate((scale_ref, product_ref)):
                for m in range(split):
                    ref[:, m * lanes : (m + 1) * lanes] = extra[n * split + m : n * split + m + 1]


def call(kernel, outs, scratch, *args, scalars=0):
    specs = [pl.BlockSpec(memory_space=pltpu.SMEM)] * scalars
    specs += [pl.BlockSpec(memory_space=pltpu.VMEM)] * (len(args) - scalars)
    return pl.pallas_call(
        kernel,
        out_shape=[jax.ShapeDtypeStruct(s, d) for s, d in outs],
        in_specs=specs,
        out_specs=[pl.BlockSpec(memory_space=pltpu.VMEM)] * len(outs),
        scratch_shapes=[pltpu.VMEM(s, d) for s, d in scratch],
        interpret=INTERPRET,
    )(*args)


def exchanged(parts, axis):
    return lax.all_to_all(parts, axis, split_axis=0, concat_axis=0, tiled=True)


def copies(own, axis):
    return exchanged(jnp.broadcast_to(own, (lax.axis_size(axis),) + own.shape), axis)


def per_device(
    saved_alignment,
    homolog_existence,
    amino_existence,
    couple_delta_adjoint,
    feedforward_adjoint,
    feedforward_scale,
    expansion_matrix,
    contraction_matrix,
    product_scale_vector,
    twin_operand_matrix,
    couple_projection_matrix,
):
    seqs, res, features = saved_alignment.shape
    units = expansion_matrix.shape[1]
    factor = twin_operand_matrix.shape[1] // 2
    pair_width = couple_projection_matrix.shape[1]
    rows = seqs * res
    row_devices, cols, cores = (lax.axis_size(a) for a in ("row", "col", "sub"))
    shards = cols * cores
    blocks = row_devices // shards
    col_res = couple_delta_adjoint.shape[1]
    all_seqs = seqs * shards
    wide = res * factor
    assert (factor, res, blocks, cores, pair_width) == (32, 32, 2, 2, lanes)
    assert col_res == blocks * res and features == 2 * lanes and units == shards * lanes
    x = saved_alignment.reshape(rows, features)
    keep = jnp.pad(
        (homolog_existence * amino_existence[None, :]).astype(f32), ((0, 0), (0, lanes - res))
    )
    scale_in = feedforward_scale.reshape(1, features)
    scale_out = product_scale_vector.reshape(1, features)
    twin = twin_operand_matrix.T
    record = wide + lanes
    (right, left, normed_in, hidden, slope, hat_in, hat_out, normed_out, spread) = call(
        forward_kernel,
        [
            ((row_devices, seqs, record), bf16),
            ((seqs, record), bf16),
            ((rows, features), bf16),
            ((rows, units), bf16),
            ((rows, units), f32),
            ((rows, features), f32),
            ((rows, features), f32),
            ((rows, features), bf16),
            ((rows, lanes), f32),
        ],
        [((rows, lanes), f32), ((seqs * factor, lanes), f32)],
        x, keep, scale_in, expansion_matrix, contraction_matrix, scale_out, twin,
    )
    right = exchanged(right, "row").reshape(shards, blocks, seqs, record)
    left = jnp.broadcast_to(left, (shards, 1, seqs, record))
    records = exchanged(jnp.concatenate([right, left], axis=1), ("col", "sub"))
    pairs = lanes // col_res
    sets = factor // pairs
    back, result_adjoint = call(
        pair_kernel,
        [((shards, blocks + 1, seqs, wide), bf16), ((sets * factor, pairs * lanes), f32)],
        [
            ((all_seqs, wide), bf16),
            ((all_seqs, col_res * factor), bf16),
            ((sets * factor, res * lanes), bf16),
            ((res * lanes, pairs * lanes), bf16),
            ((res * factor, sets * lanes), bf16),
            ((factor * factor, lanes), f32),
            ((sets * factor, pairs * lanes), bf16),
        ],
        records, couple_delta_adjoint, couple_projection_matrix,
    )
    back = exchanged(back, ("col", "sub"))
    right_back = exchanged(back[:, :blocks].reshape(row_devices, seqs, wide), "row")
    core = lax.axis_index("sub").reshape(1)
    starts = chunk_rows(rows, features, units, factor, pair_width, shards)
    lines = -(-(starts[4] + 8) // (2 * row_devices)) * 2 * row_devices
    start_adjoint, own, send = call(
        backward_kernel,
        [
            ((rows, features), bf16),
            ((cols, lines, lanes), bf16),
            ((cols, lines, lanes), bf16),
        ],
        [
            ((rows, lanes), f32),
            ((seqs * factor, lanes), f32),
            ((cores, cols, lines, lanes), bf16),
        ],
        core, back, right_back, keep, feedforward_adjoint.reshape(rows, features), scale_in,
        expansion_matrix, contraction_matrix, scale_out, twin, result_adjoint, normed_in, hidden, slope,
        hat_in, hat_out, normed_out, spread,
        scalars=1,
    )
    swap = [(0, 1), (1, 0)]
    half = (own.astype(f32) + lax.ppermute(send, "sub", swap).astype(f32)).astype(bf16)
    half = exchanged(half, "col").astype(f32).sum(axis=0).astype(bf16)
    half = exchanged(half.reshape(row_devices, -1, 2, lanes), "row").astype(f32).sum(axis=0).astype(bf16)
    half = copies(half, "row").reshape(lines, lanes)
    half = copies(half, "col")
    other = lax.ppermute(half, "sub", swap)
    grads = call(
        final_kernel,
        [
            ((factor * factor, pair_width), f32),
            ((2 * factor, features), f32),
            ((features, units), f32),
            ((units, features), f32),
            ((1, features), f32),
            ((1, features), f32),
        ],
        [],
        core, half, other,
        scalars=1,
    )
    return (
        start_adjoint.reshape(seqs, res, features),
        grads[0],
        grads[1].T,
        grads[2],
        grads[3],
        grads[4].reshape(features),
        grads[5].reshape(features),
    )


def solution(mesh):
    return jax.shard_map(
        per_device,
        mesh=mesh,
        in_specs=(
            P(("col", "sub"), ("groups", "row"), None),
            P(("col", "sub"), ("groups", "row")),
            P(("groups", "row")),
            P(("groups", "row"), ("col", "sub"), None),
            P(("col", "sub"), ("groups", "row"), None),
            P(),
            P(),
            P(),
            P(),
            P(),
            P(),
        ),
        out_specs=(
            P(("col", "sub"), ("groups", "row"), None),
            P("groups", None),
            P("groups", None),
            P("groups", None),
            P("groups", None),
            P("groups"),
            P("groups"),
        ),
        check_vma=False,
    )
```

```python
import math

import jax
import jax.numpy as jnp
from jax import lax
from jax.experimental import pallas as pl
from jax.experimental.pallas import tpu as pltpu
from jax.sharding import PartitionSpec as P

epsilon = 1e-05
lanes = 128
f32 = jnp.float32
bf16 = jnp.bfloat16
INTERPRET = False


def layer_normalize(values):
    centre = jnp.mean(values, axis=-1, keepdims=True)
    centred = values - centre
    variance = jnp.mean(centred * centred, axis=-1, keepdims=True)
    inv_std = lax.rsqrt(variance + epsilon)
    return (centred * inv_std, inv_std)


def standardizer_adjoint(grad_hat, normed, inv_std):
    first_mean = jnp.mean(grad_hat, axis=-1, keepdims=True)
    second_mean = jnp.mean(grad_hat * normed, axis=-1, keepdims=True)
    return inv_std * (grad_hat - first_mean - normed * second_mean)


def plain(a, b):
    return lax.dot_general(a, b, (((1,), (0,)), ((), ())), preferred_element_type=f32)


def last_last(a, b):
    return lax.dot_general(a, b, (((1,), (1,)), ((), ())), preferred_element_type=f32)


def first_first(a, b):
    return lax.dot_general(a, b, (((0,), (0,)), ((), ())), preferred_element_type=f32)


def turn(values, shift):
    shift = shift % lanes
    return values if shift == 0 else pltpu.roll(values, shift, 1)


def lane_index(shape):
    return lax.broadcasted_iota(jnp.int32, shape, 1)


def keep_column(keep, seqs, res):
    rows = seqs * res
    wide = jnp.broadcast_to(keep[:, None, :], (seqs, res, lanes)).reshape(rows, lanes)
    residue = lax.broadcasted_iota(jnp.int32, (rows, lanes), 0) % res
    own = lane_index((rows, lanes)) == residue
    return jnp.sum(jnp.where(own, wide, 0.0), axis=1, keepdims=True)


def forward_kernel(
    x_ref, keep_ref, scale_in_ref, w_in_ref, w_mid_ref, scale_out_ref, twin_ref,
    right_ref, left_ref, normed_in_ref, hidden_ref, slope_ref, hat_in_ref, hat_out_ref,
    normed_out_ref, spread_ref, left_rows, right_rows,
):
    seqs = keep_ref.shape[0]
    rows = x_ref.shape[0]
    res = rows // seqs
    factor = twin_ref.shape[0] // 2
    group = lanes // factor
    x = x_ref[...].astype(f32)
    hat_in, inv_in = layer_normalize(x)
    hat_in_ref[...] = hat_in
    normed_in = (hat_in * scale_in_ref[...]).astype(bf16)
    normed_in_ref[...] = normed_in
    pre = plain(normed_in, w_in_ref[...])
    share = 0.5 * (1.0 + lax.erf(pre * math.sqrt(0.5)))
    hidden = (pre * share).astype(bf16)
    hidden_ref[...] = hidden
    slope_ref[...] = share + pre * (jnp.exp(-0.5 * pre * pre) * (1.0 / math.sqrt(2.0 * math.pi)))
    mixed = x + plain(hidden, w_mid_ref[...])
    hat_out, inv_out = layer_normalize(mixed)
    hat_out_ref[...] = hat_out
    lane = lane_index((rows, lanes))
    spread_ref[...] = jnp.where(lane == 0, inv_in, inv_out)
    normed_out = (hat_out * scale_out_ref[...]).astype(bf16)
    normed_out_ref[...] = normed_out
    keep = keep_ref[...]
    twin = twin_ref[...]
    projected = last_last(
        normed_out, jnp.concatenate([twin, jnp.zeros((lanes - 2 * factor, twin.shape[1]), bf16)], axis=0)
    )
    left_rows[...] = jnp.where(lane < factor, projected * keep_column(keep, seqs, res), 0.0)
    turned = last_last(twin[factor:], normed_out)
    per = lanes // res
    for s in range(seqs):
        tile = turned[:, (s // per) * lanes : (s // per + 1) * lanes]
        right_rows[s * factor : (s + 1) * factor, :] = turn(tile, -(s % per) * res)
    for t in range(res // group):
        tile = left_rows[pl.ds(t * group, seqs, stride=res), :]
        for m in range(1, group):
            tile = tile + turn(left_rows[pl.ds(t * group + m, seqs, stride=res), :], m * factor)
        left_ref[:, t * lanes : (t + 1) * lanes] = tile.astype(bf16)
    left_ref[:, res * factor :] = keep.astype(bf16)
    pieces = []
    for t in range(factor // per):
        tile = right_rows[pl.ds(t * per, seqs, stride=factor), :] * keep
        for m in range(1, per):
            piece = right_rows[pl.ds(t * per + m, seqs, stride=factor), :] * keep
            tile = tile + turn(piece, m * res)
        pieces.append(tile)
    record = jnp.concatenate(pieces + [keep], axis=1).astype(bf16)
    for c in range(right_ref.shape[0]):
        right_ref[c] = record


def pair_kernel(
    parity_ref, rec_ref, other_ref, cot_ref, proj_ref, own_ref, send_ref, back_ref, grad_ref,
    left_all, right_all, outer_all, adjoint_all, pulled_all, proj_rows, proj_all,
):
    shards, _, seqs, _ = rec_ref.shape
    blocks = 2
    even = parity_ref[0] == 0
    all_seqs = shards * seqs
    res = cot_ref.shape[0]
    cols = cot_ref.shape[1]
    wide = back_ref.shape[2]
    factor = wide // res
    pairs = lanes // cols
    sets = factor // pairs
    half = cols // blocks
    lane = lane_index((all_seqs, lanes))

    def left_tile(t):
        return rec_ref[:, 1, :, t * lanes : (t + 1) * lanes].astype(f32).reshape(all_seqs, lanes)

    def right_tiles(t):
        own = rec_ref[:, 0, :, t * lanes : (t + 1) * lanes].astype(f32).reshape(all_seqs, lanes)
        other = other_ref[:, :, t * lanes : (t + 1) * lanes].astype(f32).reshape(all_seqs, lanes)
        return jnp.where(even, own, other), jnp.where(even, other, own)

    for t in range(wide // lanes):
        left_all[:, t * lanes : (t + 1) * lanes] = left_tile(t).astype(bf16)
        a, b = right_tiles(t)
        first = jnp.where(
            lane < 32, a, jnp.where(lane < 64, turn(b, 32), jnp.where(lane < 96, turn(a, 32), turn(b, 64)))
        )
        second = jnp.where(
            lane < 32, turn(a, 64), jnp.where(lane < 64, turn(b, 96), jnp.where(lane < 96, turn(a, 96), b))
        )
        right_all[:, 2 * t * lanes : (2 * t + 1) * lanes] = first.astype(bf16)
        right_all[:, (2 * t + 1) * lanes : (2 * t + 2) * lanes] = second.astype(bf16)
    last = wide // lanes
    keep_rows = left_tile(last).astype(bf16)
    a, b = right_tiles(last)
    keep_cols = (a + turn(b, half)).astype(bf16)
    count = first_first(keep_cols, keep_rows)[:cols]
    inverse = 1.0 / jnp.maximum(count, 1.0)
    nothing = jnp.zeros((cols, lanes), bf16)
    for i in range(res):
        scaled = (cot_ref[i].astype(f32) * inverse[:, i : i + 1]).astype(bf16)
        at = i * lanes
        for k in range(pairs):
            for m in range(pairs):
                adjoint_all[at + k * cols : at + (k + 1) * cols, m * lanes : (m + 1) * lanes] = (
                    scaled if k == m else nothing
                )
    proj_rows[...] = proj_ref[...].astype(f32)
    for n in range(sets):
        for k in range(pairs):
            proj_all[n * factor : (n + 1) * factor, k * lanes : (k + 1) * lanes] = proj_rows[
                pl.ds(n * pairs + k, factor, stride=factor), :
            ].astype(bf16)
    step = 256 // factor
    for c in range(res // step):
        outer = first_first(left_all[:, c * step * factor : (c + 1) * step * factor], right_all[...])
        for i in range(step):
            at = (c * step + i) * lanes
            for n in range(sets):
                outer_all[n * factor : (n + 1) * factor, at : at + lanes] = outer[
                    i * factor : (i + 1) * factor, n * lanes : (n + 1) * lanes
                ].astype(bf16)
        pulled = last_last(proj_all[...], adjoint_all[c * step * lanes : (c + 1) * step * lanes, :])
        for i in range(step):
            at = (c * step + i) * factor
            for n in range(sets):
                pulled_all[at : at + factor, n * lanes : (n + 1) * lanes] = pulled[
                    n * factor : (n + 1) * factor, i * lanes : (i + 1) * lanes
                ].astype(bf16)
    grad_ref[...] = plain(outer_all[...], adjoint_all[...])
    grad_left = last_last(right_all[...], pulled_all[...])
    grad_right = plain(left_all[...], pulled_all[...])

    def put(ref, t, values):
        ref[:, :, t * lanes : (t + 1) * lanes] = values.reshape(shards, seqs, lanes).astype(bf16)

    for t in range(wide // lanes):
        put(back_ref, t, grad_left[:, t * lanes : (t + 1) * lanes])
        a = grad_right[:, 2 * t * lanes : (2 * t + 1) * lanes]
        b = grad_right[:, (2 * t + 1) * lanes : (2 * t + 2) * lanes]
        first = jnp.where(
            lane < 32, a, jnp.where(lane < 64, turn(a, 96), jnp.where(lane < 96, turn(b, 64), turn(b, 32)))
        )
        second = jnp.where(
            lane < 32, turn(a, 96), jnp.where(lane < 64, turn(a, 64), jnp.where(lane < 96, turn(b, 32), b))
        )
        put(own_ref, t, jnp.where(even, first, second))
        put(send_ref, t, jnp.where(even, second, first))


def chunk_rows(rows, features, hidden, factor, pair_width, chunks):
    sizes = (
        features * hidden // chunks // lanes,
        hidden * features // chunks // lanes,
        factor * factor * pair_width // chunks // lanes,
        2 * factor * features // chunks // lanes,
    )
    starts = [0]
    for size in sizes:
        starts.append(starts[-1] + size)
    return starts


def backward_kernel(
    core_ref, left_ref, right_ref, keep_ref, cot_ref, scale_in_ref, w_in_ref, w_mid_ref, scale_out_ref,
    twin_ref, grad_ref, normed_in_ref, hidden_ref, slope_ref, hat_in_ref, hat_out_ref, normed_out_ref,
    spread_ref, out_ref, own_ref, send_ref, left_rows, right_rows, chunks_ref,
):
    seqs = keep_ref.shape[0]
    rows, features = cot_ref.shape
    res = rows // seqs
    factor = twin_ref.shape[0] // 2
    group = lanes // factor
    per = lanes // res
    cols = own_ref.shape[0]
    chunks = 2 * cols
    units = hidden_ref.shape[1]
    pair_width = lanes
    starts = chunk_rows(rows, features, units, factor, pair_width, chunks)
    keep = keep_ref[...]
    lane_small = lane_index((seqs, lanes))
    last = left_ref.shape[1] - 1
    for t in range(res // group):
        tile = jnp.sum(left_ref[:, last, :, t * lanes : (t + 1) * lanes].astype(f32), axis=0)
        for m in range(group):
            piece = jnp.where(lane_small < factor, turn(tile, -m * factor), 0.0)
            left_rows[pl.ds(t * group + m, seqs, stride=res), :] = piece
    for t in range(factor // per):
        tile = jnp.sum(right_ref[:, :, t * lanes : (t + 1) * lanes].astype(f32), axis=0)
        for m in range(per):
            right_rows[pl.ds(t * per + m, seqs, stride=factor), :] = turn(tile, -m * res) * keep
    tiles = []
    for h in range(rows // lanes):
        tile = right_rows[h * per * factor : (h * per + 1) * factor, :]
        for m in range(1, per):
            at = (h * per + m) * factor
            tile = tile + turn(right_rows[at : at + factor, :], m * res)
        tiles.append(tile)
    turned = jnp.concatenate(tiles, axis=1)
    turned = jnp.concatenate(
        [jnp.zeros((factor, rows), f32), turned, jnp.zeros((lanes - 2 * factor, rows), f32)], axis=0
    )
    grad_proj = (left_rows[...] * keep_column(keep, seqs, res) + jnp.transpose(turned)).astype(bf16)
    twin = twin_ref[...]
    twin = jnp.concatenate([twin, jnp.zeros((lanes - 2 * factor, features), bf16)], axis=0)
    operand_adjoint = first_first(grad_proj, normed_out_ref[...])
    rescaled = plain(grad_proj, twin)
    hat_out = hat_out_ref[...]
    product_adjoint = jnp.sum(rescaled * hat_out, axis=0, keepdims=True)
    inv_in = spread_ref[:, 0:1]
    inv_out = spread_ref[:, 1:2]
    combined = cot_ref[...].astype(f32) + standardizer_adjoint(
        rescaled * scale_out_ref[...], hat_out, inv_out
    )
    mixed_half = combined.astype(bf16)
    grad_hidden = last_last(mixed_half, w_mid_ref[...])
    grad_pre = (slope_ref[...] * grad_hidden).astype(bf16)
    grad_in = last_last(grad_pre, w_in_ref[...])
    hat_in = hat_in_ref[...]
    scale_adjoint = jnp.sum(grad_in * hat_in, axis=0, keepdims=True)
    out_ref[...] = (
        combined + standardizer_adjoint(grad_in * scale_in_ref[...], hat_in, inv_in)
    ).astype(bf16)
    hidden_adjoint = first_first(hidden_ref[...], mixed_half)
    expansion_adjoint = first_first(normed_in_ref[...], grad_pre)
    split = features // lanes

    def put(k, at, values):
        chunks_ref[k // cols, k % cols, at : at + values.shape[0], :] = values.astype(bf16)

    unit_step = units // chunks
    for k in range(chunks):
        put(k, starts[0], expansion_adjoint[:, k * unit_step : (k + 1) * unit_step])
        for m in range(split):
            put(k, starts[1] + m * unit_step,
                hidden_adjoint[k * unit_step : (k + 1) * unit_step, m * lanes : (m + 1) * lanes])
        height = grad_ref.shape[0] // chunks
        for m in range(grad_ref.shape[1] // lanes):
            put(k, starts[2] + m * height, grad_ref[k * height : (k + 1) * height, m * lanes : (m + 1) * lanes])
        height = 2 * factor // chunks
        tail = [
            operand_adjoint[k * height : (k + 1) * height, m * lanes : (m + 1) * lanes] for m in range(split)
        ]
        row = lax.broadcasted_iota(jnp.int32, (8, lanes), 0)
        extra = jnp.zeros((8, lanes), f32)
        if k == 0:
            for n, vector in enumerate((scale_adjoint, product_adjoint)):
                for m in range(split):
                    extra = jnp.where(row == n * split + m, vector[:, m * lanes : (m + 1) * lanes], extra)
        rest = chunks_ref.shape[2] - starts[4] - 8
        block = jnp.concatenate(tail + [extra, jnp.zeros((rest, lanes), f32)], axis=0)
        put(k, starts[3], block)
    core = core_ref[0]
    own_ref[...] = chunks_ref[core]
    send_ref[...] = chunks_ref[1 - core]


def final_kernel(
    core_ref, half_ref, other_ref, grad_ref, twin_ref, w_in_ref, w_mid_ref, scale_ref, product_ref
):
    cols = half_ref.shape[0]
    chunks = 2 * cols
    features, units = w_in_ref.shape
    factor = twin_ref.shape[0] // 2
    starts = chunk_rows(0, features, units, factor, lanes, chunks)
    split = features // lanes
    unit_step = units // chunks
    core = core_ref[0]
    height = factor * factor // 2 // chunks
    for k in range(chunks):
        mine = core == k // cols

        def read(at, size):
            return jnp.where(
                mine,
                half_ref[k % cols, at : at + size, :].astype(f32),
                other_ref[k % cols, at : at + size, :].astype(f32),
            )

        w_in_ref[:, k * unit_step : (k + 1) * unit_step] = read(starts[0], features)
        for m in range(split):
            w_mid_ref[k * unit_step : (k + 1) * unit_step, m * lanes : (m + 1) * lanes] = read(
                starts[1] + m * unit_step, unit_step
            )
        for m in range(2):
            block = read(starts[2] + m * height, height)
            for n in range(height // factor):
                q = 2 * (k * (height // factor) + n) + m
                grad_ref[pl.ds(q, factor, stride=factor), :] = block[n * factor : (n + 1) * factor]
        tall = 2 * factor // chunks
        block = read(starts[3], starts[4] - starts[3])
        for m in range(split):
            twin_ref[k * tall : (k + 1) * tall, m * lanes : (m + 1) * lanes] = block[m * tall : (m + 1) * tall]
        if k == 0:
            extra = read(starts[4], 8)
            for n, ref in enumerate((scale_ref, product_ref)):
                for m in range(split):
                    ref[:, m * lanes : (m + 1) * lanes] = extra[n * split + m : n * split + m + 1]


def call(kernel, outs, scratch, *args, scalars=0):
    specs = [pl.BlockSpec(memory_space=pltpu.SMEM)] * scalars
    specs += [pl.BlockSpec(memory_space=pltpu.VMEM)] * (len(args) - scalars)
    return pl.pallas_call(
        kernel,
        out_shape=[jax.ShapeDtypeStruct(s, d) for s, d in outs],
        in_specs=specs,
        out_specs=[pl.BlockSpec(memory_space=pltpu.VMEM)] * len(outs),
        scratch_shapes=[pltpu.VMEM(s, d) for s, d in scratch],
        interpret=INTERPRET,
    )(*args)


def exchanged(parts, axis, groups=None):
    return lax.all_to_all(
        parts, axis, split_axis=0, concat_axis=0, axis_index_groups=groups, tiled=True
    )


def copies(own, axis, groups):
    return exchanged(jnp.broadcast_to(own, (len(groups[0]),) + own.shape), axis, groups)


def per_device(
    saved_alignment,
    homolog_existence,
    amino_existence,
    couple_delta_adjoint,
    feedforward_adjoint,
    feedforward_scale,
    expansion_matrix,
    contraction_matrix,
    product_scale_vector,
    twin_operand_matrix,
    couple_projection_matrix,
):
    seqs, res, features = saved_alignment.shape
    units = expansion_matrix.shape[1]
    factor = twin_operand_matrix.shape[1] // 2
    pair_width = couple_projection_matrix.shape[1]
    rows = seqs * res
    row_devices, cols, cores = (lax.axis_size(a) for a in ("row", "col", "sub"))
    shards = cols * cores
    blocks = row_devices // shards
    col_res = couple_delta_adjoint.shape[1]
    all_seqs = seqs * shards
    wide = res * factor
    assert (factor, res, blocks, cores, pair_width) == (32, 32, 2, 2, lanes)
    assert col_res == blocks * res and features == 2 * lanes and units == shards * lanes
    x = saved_alignment.reshape(rows, features)
    keep = jnp.pad(
        (homolog_existence * amino_existence[None, :]).astype(f32), ((0, 0), (0, lanes - res))
    )
    scale_in = feedforward_scale.reshape(1, features)
    scale_out = product_scale_vector.reshape(1, features)
    twin = twin_operand_matrix.T
    record = wide + lanes
    (right, left, normed_in, hidden, slope, hat_in, hat_out, normed_out, spread) = call(
        forward_kernel,
        [
            ((row_devices // 2, seqs, record), bf16),
            ((seqs, record), bf16),
            ((rows, features), bf16),
            ((rows, units), bf16),
            ((rows, units), f32),
            ((rows, features), f32),
            ((rows, features), f32),
            ((rows, features), bf16),
            ((rows, lanes), f32),
        ],
        [((rows, lanes), f32), ((seqs * factor, lanes), f32)],
        x, keep, scale_in, expansion_matrix, contraction_matrix, scale_out, twin,
    )
    alike = [list(range(b, row_devices, 2)) for b in range(2)]
    swap_rows = [(i, i ^ 1) for i in range(row_devices)]
    parity = (lax.axis_index("row") % 2).reshape(1)
    right = exchanged(right, "row", alike)
    records = exchanged(
        jnp.stack([right, jnp.broadcast_to(left, (shards, seqs, record))], axis=1), ("col", "sub")
    )
    other = lax.ppermute(records[:, 0], "row", swap_rows)
    pairs = lanes // col_res
    sets = factor // pairs
    own, send, left, result_adjoint = call(
        pair_kernel,
        [
            ((shards, seqs, wide), bf16),
            ((shards, seqs, wide), bf16),
            ((shards, seqs, wide), bf16),
            ((sets * factor, pairs * lanes), f32),
        ],
        [
            ((all_seqs, wide), bf16),
            ((all_seqs, col_res * factor), bf16),
            ((sets * factor, res * lanes), bf16),
            ((res * lanes, pairs * lanes), bf16),
            ((res * factor, sets * lanes), bf16),
            ((factor * factor, lanes), f32),
            ((sets * factor, pairs * lanes), bf16),
        ],
        parity, records, other, couple_delta_adjoint, couple_projection_matrix,
        scalars=1,
    )
    own = (own.astype(f32) + lax.ppermute(send, "row", swap_rows).astype(f32)).astype(bf16)
    back = exchanged(jnp.stack([own, left], axis=1), ("col", "sub"))
    right_back = exchanged(back[:, 0], "row", alike)
    core = lax.axis_index("sub").reshape(1)
    starts = chunk_rows(rows, features, units, factor, pair_width, shards)
    lines = -(-(starts[4] + 8) // (2 * row_devices)) * 2 * row_devices
    start_adjoint, own, send = call(
        backward_kernel,
        [
            ((rows, features), bf16),
            ((cols, lines, lanes), bf16),
            ((cols, lines, lanes), bf16),
        ],
        [
            ((rows, lanes), f32),
            ((seqs * factor, lanes), f32),
            ((cores, cols, lines, lanes), bf16),
        ],
        core, back, right_back, keep, feedforward_adjoint.reshape(rows, features), scale_in,
        expansion_matrix, contraction_matrix, scale_out, twin, result_adjoint, normed_in, hidden, slope,
        hat_in, hat_out, normed_out, spread,
        scalars=1,
    )
    swap = [(0, 1), (1, 0)]
    half = (own.astype(f32) + lax.ppermute(send, "sub", swap).astype(f32)).astype(bf16)
    near = [
        [(2 * m + b) * cols + c for c in range(cols) for b in range(2)] for m in range(row_devices // 2)
    ]
    half = exchanged(half.reshape(2 * cols, lines // 2, lanes), ("row", "col"), near)
    half = half.astype(f32).sum(axis=0).astype(bf16)
    half = exchanged(half.reshape(row_devices // 2, -1, 2, lanes), "row", alike)
    half = half.astype(f32).sum(axis=0).astype(bf16)
    half = copies(half, "row", alike).reshape(lines // 2, lanes)
    half = copies(half, ("row", "col"), near).reshape(cols, lines, lanes)
    other = lax.ppermute(half, "sub", swap)
    grads = call(
        final_kernel,
        [
            ((factor * factor, pair_width), f32),
            ((2 * factor, features), f32),
            ((features, units), f32),
            ((units, features), f32),
            ((1, features), f32),
            ((1, features), f32),
        ],
        [],
        core, half, other,
        scalars=1,
    )
    return (
        start_adjoint.reshape(seqs, res, features),
        grads[0],
        grads[1].T,
        grads[2],
        grads[3],
        grads[4].reshape(features),
        grads[5].reshape(features),
    )


def solution(mesh):
    return jax.shard_map(
        per_device,
        mesh=mesh,
        in_specs=(
            P(("col", "sub"), ("groups", "row"), None),
            P(("col", "sub"), ("groups", "row")),
            P(("groups", "row")),
            P(("groups", "row"), ("col", "sub"), None),
            P(("col", "sub"), ("groups", "row"), None),
            P(),
            P(),
            P(),
            P(),
            P(),
            P(),
        ),
        out_specs=(
            P(("col", "sub"), ("groups", "row"), None),
            P("groups", None),
            P("groups", None),
            P("groups", None),
            P("groups", None),
            P("groups"),
            P("groups"),
        ),
        check_vma=False,
    )
```

```python
import math

import jax
import jax.numpy as jnp
from jax import lax
from jax.experimental import pallas as pl
from jax.experimental.pallas import tpu as pltpu
from jax.sharding import PartitionSpec as P

epsilon = 1e-05
lanes = 128
f32 = jnp.float32
bf16 = jnp.bfloat16
INTERPRET = False


def layer_normalize(values):
    centre = jnp.mean(values, axis=-1, keepdims=True)
    centred = values - centre
    variance = jnp.mean(centred * centred, axis=-1, keepdims=True)
    inv_std = lax.rsqrt(variance + epsilon)
    return (centred * inv_std, inv_std)


def standardizer_adjoint(grad_hat, normed, inv_std):
    first_mean = jnp.mean(grad_hat, axis=-1, keepdims=True)
    second_mean = jnp.mean(grad_hat * normed, axis=-1, keepdims=True)
    return inv_std * (grad_hat - first_mean - normed * second_mean)


def plain(a, b):
    return lax.dot_general(a, b, (((1,), (0,)), ((), ())), preferred_element_type=f32)


def last_last(a, b):
    return lax.dot_general(a, b, (((1,), (1,)), ((), ())), preferred_element_type=f32)


def first_first(a, b):
    return lax.dot_general(a, b, (((0,), (0,)), ((), ())), preferred_element_type=f32)


def turn(values, shift):
    shift = shift % lanes
    return values if shift == 0 else pltpu.roll(values, shift, 1)


def lane_index(shape):
    return lax.broadcasted_iota(jnp.int32, shape, 1)


def keep_column(keep, seqs, res):
    rows = seqs * res
    wide = jnp.broadcast_to(keep[:, None, :], (seqs, res, lanes)).reshape(rows, lanes)
    residue = lax.broadcasted_iota(jnp.int32, (rows, lanes), 0) % res
    own = lane_index((rows, lanes)) == residue
    return jnp.sum(jnp.where(own, wide, 0.0), axis=1, keepdims=True)


def forward_kernel(
    x_ref, present_ref, residue_ref, scale_in_ref, w_in_ref, w_mid_ref, scale_out_ref, twin_ref,
    keep_ref, right_ref, left_ref, normed_in_ref, hidden_ref, slope_ref, hat_in_ref, hat_out_ref,
    normed_out_ref, spread_ref, left_rows, right_rows,
):
    seqs, res = present_ref.shape
    rows = x_ref.shape[0]
    keep_ref[...] = jnp.zeros((seqs, lanes), f32)
    keep_ref[:, :res] = (present_ref[...] * residue_ref[...]).astype(f32)
    factor = twin_ref.shape[0] // 2
    group = lanes // factor
    x = x_ref[...].astype(f32)
    hat_in, inv_in = layer_normalize(x)
    hat_in_ref[...] = hat_in
    normed_in = (hat_in * scale_in_ref[...]).astype(bf16)
    normed_in_ref[...] = normed_in
    pre = plain(normed_in, w_in_ref[...])
    share = 0.5 * (1.0 + lax.erf(pre * math.sqrt(0.5)))
    hidden = (pre * share).astype(bf16)
    hidden_ref[...] = hidden
    slope_ref[...] = share + pre * (jnp.exp(-0.5 * pre * pre) * (1.0 / math.sqrt(2.0 * math.pi)))
    mixed = x + plain(hidden, w_mid_ref[...])
    hat_out, inv_out = layer_normalize(mixed)
    hat_out_ref[...] = hat_out
    lane = lane_index((rows, lanes))
    spread_ref[...] = jnp.where(lane == 0, inv_in, inv_out)
    normed_out = (hat_out * scale_out_ref[...]).astype(bf16)
    normed_out_ref[...] = normed_out
    keep = keep_ref[...]
    twin = twin_ref[...]
    projected = last_last(
        normed_out, jnp.concatenate([twin, jnp.zeros((lanes - 2 * factor, twin.shape[1]), bf16)], axis=0)
    )
    left_rows[...] = jnp.where(lane < factor, projected * keep_column(keep, seqs, res), 0.0)
    turned = last_last(twin[factor:], normed_out)
    per = lanes // res
    for s in range(seqs):
        tile = turned[:, (s // per) * lanes : (s // per + 1) * lanes]
        right_rows[s * factor : (s + 1) * factor, :] = turn(tile, -(s % per) * res)
    left_pieces = []
    for t in range(res // group):
        tile = left_rows[pl.ds(t * group, seqs, stride=res), :]
        for m in range(1, group):
            tile = tile + turn(left_rows[pl.ds(t * group + m, seqs, stride=res), :], m * factor)
        left_pieces.append(tile)
    left_record = jnp.concatenate(left_pieces + [keep], axis=1).astype(bf16)
    for c in range(left_ref.shape[0]):
        left_ref[c] = left_record
    pieces = []
    for t in range(factor // per):
        tile = right_rows[pl.ds(t * per, seqs, stride=factor), :] * keep
        for m in range(1, per):
            piece = right_rows[pl.ds(t * per + m, seqs, stride=factor), :] * keep
            tile = tile + turn(piece, m * res)
        pieces.append(tile)
    record = jnp.concatenate(pieces + [keep], axis=1).astype(bf16)
    for c in range(right_ref.shape[0]):
        right_ref[c] = record


def pair_kernel(
    parity_ref, rec_ref, other_ref, cot_ref, proj_ref, own_ref, send_ref, back_ref, grad_ref,
    left_all, right_all, outer_all, adjoint_all, pulled_all, proj_rows, proj_all, other_all, sem,
):
    shards, seqs, record = other_ref.shape
    start = pltpu.make_async_copy(other_ref, other_all, sem)
    start.start()
    blocks = 2
    even = parity_ref[0] == 0
    all_seqs = shards * seqs
    res = cot_ref.shape[0]
    cols = cot_ref.shape[1]
    wide = back_ref.shape[2]
    factor = wide // res
    pairs = lanes // cols
    sets = factor // pairs
    half = cols // blocks
    lane = lane_index((all_seqs, lanes))

    def left_tile(t):
        at = record + t * lanes
        return rec_ref[:, :, at : at + lanes].astype(f32).reshape(all_seqs, lanes)

    def right_tiles(t):
        own = rec_ref[:, :, t * lanes : (t + 1) * lanes].astype(f32).reshape(all_seqs, lanes)
        other = other_all[:, :, t * lanes : (t + 1) * lanes].astype(f32).reshape(all_seqs, lanes)
        return jnp.where(even, own, other), jnp.where(even, other, own)

    proj_rows[...] = proj_ref[...].astype(f32)
    for n in range(sets):
        for k in range(pairs):
            proj_all[n * factor : (n + 1) * factor, k * lanes : (k + 1) * lanes] = proj_rows[
                pl.ds(n * pairs + k, factor, stride=factor), :
            ].astype(bf16)
    for t in range(wide // lanes):
        left_all[:, t * lanes : (t + 1) * lanes] = left_tile(t).astype(bf16)
    start.wait()
    for t in range(wide // lanes):
        a, b = right_tiles(t)
        first = jnp.where(
            lane < 32, a, jnp.where(lane < 64, turn(b, 32), jnp.where(lane < 96, turn(a, 32), turn(b, 64)))
        )
        second = jnp.where(
            lane < 32, turn(a, 64), jnp.where(lane < 64, turn(b, 96), jnp.where(lane < 96, turn(a, 96), b))
        )
        right_all[:, 2 * t * lanes : (2 * t + 1) * lanes] = first.astype(bf16)
        right_all[:, (2 * t + 1) * lanes : (2 * t + 2) * lanes] = second.astype(bf16)
    last = wide // lanes
    keep_rows = left_tile(last).astype(bf16)
    a, b = right_tiles(last)
    keep_cols = (a + turn(b, half)).astype(bf16)
    count = first_first(keep_cols, keep_rows)[:cols]
    inverse = 1.0 / jnp.maximum(count, 1.0)
    nothing = jnp.zeros((cols, lanes), bf16)
    for i in range(res):
        scaled = (cot_ref[i].astype(f32) * inverse[:, i : i + 1]).astype(bf16)
        at = i * lanes
        for k in range(pairs):
            for m in range(pairs):
                adjoint_all[at + k * cols : at + (k + 1) * cols, m * lanes : (m + 1) * lanes] = (
                    scaled if k == m else nothing
                )
    step = 256 // factor
    for c in range(res // step):
        outer = first_first(left_all[:, c * step * factor : (c + 1) * step * factor], right_all[...])
        for i in range(step):
            at = (c * step + i) * lanes
            for n in range(sets):
                outer_all[n * factor : (n + 1) * factor, at : at + lanes] = outer[
                    i * factor : (i + 1) * factor, n * lanes : (n + 1) * lanes
                ].astype(bf16)
        pulled = last_last(proj_all[...], adjoint_all[c * step * lanes : (c + 1) * step * lanes, :])
        for i in range(step):
            at = (c * step + i) * factor
            for n in range(sets):
                pulled_all[at : at + factor, n * lanes : (n + 1) * lanes] = pulled[
                    n * factor : (n + 1) * factor, i * lanes : (i + 1) * lanes
                ].astype(bf16)
    grad_ref[...] = plain(outer_all[...], adjoint_all[...])
    grad_left = last_last(right_all[...], pulled_all[...])
    grad_right = plain(left_all[...], pulled_all[...])

    def put(ref, t, values):
        ref[:, :, t * lanes : (t + 1) * lanes] = values.reshape(shards, seqs, lanes).astype(bf16)

    for t in range(wide // lanes):
        put(back_ref, t, grad_left[:, t * lanes : (t + 1) * lanes])
        a = grad_right[:, 2 * t * lanes : (2 * t + 1) * lanes]
        b = grad_right[:, (2 * t + 1) * lanes : (2 * t + 2) * lanes]
        first = jnp.where(
            lane < 32, a, jnp.where(lane < 64, turn(a, 96), jnp.where(lane < 96, turn(b, 64), turn(b, 32)))
        )
        second = jnp.where(
            lane < 32, turn(a, 96), jnp.where(lane < 64, turn(a, 64), jnp.where(lane < 96, turn(b, 32), b))
        )
        put(own_ref, t, jnp.where(even, first, second))
        put(send_ref, t, jnp.where(even, second, first))


def chunk_rows(rows, features, hidden, factor, pair_width, chunks):
    sizes = (
        features * hidden // chunks // lanes,
        hidden * features // chunks // lanes,
        factor * factor * pair_width // chunks // lanes,
        2 * factor * features // chunks // lanes,
    )
    starts = [0]
    for size in sizes:
        starts.append(starts[-1] + size)
    return starts


def backward_kernel(
    core_ref, left_ref, right_ref, keep_ref, cot_ref, scale_in_ref, w_in_ref, w_mid_ref, scale_out_ref,
    twin_ref, grad_ref, normed_in_ref, hidden_ref, slope_ref, hat_in_ref, hat_out_ref, normed_out_ref,
    spread_ref, out_ref, own_ref, send_ref, left_rows, right_rows, chunks_ref, right_all, sem,
):
    start = pltpu.make_async_copy(right_ref, right_all, sem)
    start.start()
    seqs = keep_ref.shape[0]
    rows, features = cot_ref.shape
    res = rows // seqs
    factor = twin_ref.shape[0] // 2
    group = lanes // factor
    per = lanes // res
    cols = own_ref.shape[0]
    chunks = 2 * cols
    units = hidden_ref.shape[1]
    pair_width = lanes
    starts = chunk_rows(rows, features, units, factor, pair_width, chunks)
    keep = keep_ref[...]
    lane_small = lane_index((seqs, lanes))
    half = res * factor
    for t in range(res // group):
        tile = jnp.sum(left_ref[:, :, half + t * lanes : half + (t + 1) * lanes].astype(f32), axis=0)
        for m in range(group):
            piece = jnp.where(lane_small < factor, turn(tile, -m * factor), 0.0)
            left_rows[pl.ds(t * group + m, seqs, stride=res), :] = piece
    start.wait()
    for t in range(factor // per):
        tile = jnp.sum(right_all[:, :, t * lanes : (t + 1) * lanes].astype(f32), axis=0)
        for m in range(per):
            right_rows[pl.ds(t * per + m, seqs, stride=factor), :] = turn(tile, -m * res) * keep
    tiles = []
    for h in range(rows // lanes):
        tile = right_rows[h * per * factor : (h * per + 1) * factor, :]
        for m in range(1, per):
            at = (h * per + m) * factor
            tile = tile + turn(right_rows[at : at + factor, :], m * res)
        tiles.append(tile)
    turned = jnp.concatenate(tiles, axis=1)
    turned = jnp.concatenate(
        [jnp.zeros((factor, rows), f32), turned, jnp.zeros((lanes - 2 * factor, rows), f32)], axis=0
    )
    grad_proj = (left_rows[...] * keep_column(keep, seqs, res) + jnp.transpose(turned)).astype(bf16)
    twin = twin_ref[...]
    twin = jnp.concatenate([twin, jnp.zeros((lanes - 2 * factor, features), bf16)], axis=0)
    operand_adjoint = first_first(grad_proj, normed_out_ref[...])
    rescaled = plain(grad_proj, twin)
    hat_out = hat_out_ref[...]
    product_adjoint = jnp.sum(rescaled * hat_out, axis=0, keepdims=True)
    inv_in = spread_ref[:, 0:1]
    inv_out = spread_ref[:, 1:2]
    combined = cot_ref[...].astype(f32) + standardizer_adjoint(
        rescaled * scale_out_ref[...], hat_out, inv_out
    )
    mixed_half = combined.astype(bf16)
    grad_hidden = last_last(mixed_half, w_mid_ref[...])
    grad_pre = (slope_ref[...] * grad_hidden).astype(bf16)
    grad_in = last_last(grad_pre, w_in_ref[...])
    hat_in = hat_in_ref[...]
    scale_adjoint = jnp.sum(grad_in * hat_in, axis=0, keepdims=True)
    out_ref[...] = (
        combined + standardizer_adjoint(grad_in * scale_in_ref[...], hat_in, inv_in)
    ).astype(bf16)
    hidden_adjoint = first_first(hidden_ref[...], mixed_half)
    expansion_adjoint = first_first(normed_in_ref[...], grad_pre)
    split = features // lanes

    def put(k, at, values):
        chunks_ref[k // cols, k % cols, at : at + values.shape[0], :] = values.astype(bf16)

    unit_step = units // chunks
    for k in range(chunks):
        put(k, starts[0], expansion_adjoint[:, k * unit_step : (k + 1) * unit_step])
        for m in range(split):
            put(k, starts[1] + m * unit_step,
                hidden_adjoint[k * unit_step : (k + 1) * unit_step, m * lanes : (m + 1) * lanes])
        height = grad_ref.shape[0] // chunks
        for m in range(grad_ref.shape[1] // lanes):
            put(k, starts[2] + m * height, grad_ref[k * height : (k + 1) * height, m * lanes : (m + 1) * lanes])
        height = 2 * factor // chunks
        tail = [
            operand_adjoint[k * height : (k + 1) * height, m * lanes : (m + 1) * lanes] for m in range(split)
        ]
        row = lax.broadcasted_iota(jnp.int32, (8, lanes), 0)
        extra = jnp.zeros((8, lanes), f32)
        if k == 0:
            for n, vector in enumerate((scale_adjoint, product_adjoint)):
                for m in range(split):
                    extra = jnp.where(row == n * split + m, vector[:, m * lanes : (m + 1) * lanes], extra)
        rest = chunks_ref.shape[2] - starts[4] - 8
        block = jnp.concatenate(tail + [extra, jnp.zeros((rest, lanes), f32)], axis=0)
        put(k, starts[3], block)
    core = core_ref[0]
    own_ref[...] = chunks_ref[core]
    send_ref[...] = chunks_ref[1 - core]


def final_kernel(
    core_ref, half_ref, other_ref, grad_ref, twin_ref, w_in_ref, w_mid_ref, scale_ref, product_ref,
    other_all, sem,
):
    start = pltpu.make_async_copy(other_ref, other_all, sem)
    start.start()
    start.wait()
    cols = half_ref.shape[0]
    chunks = 2 * cols
    features, units = w_in_ref.shape
    factor = twin_ref.shape[0] // 2
    starts = chunk_rows(0, features, units, factor, lanes, chunks)
    split = features // lanes
    unit_step = units // chunks
    core = core_ref[0]
    height = factor * factor // 2 // chunks
    for k in range(chunks):
        mine = core == k // cols

        def read(at, size):
            return jnp.where(
                mine,
                half_ref[k % cols, at : at + size, :].astype(f32),
                other_all[k % cols, at : at + size, :].astype(f32),
            )

        w_in_ref[:, k * unit_step : (k + 1) * unit_step] = read(starts[0], features)
        for m in range(split):
            w_mid_ref[k * unit_step : (k + 1) * unit_step, m * lanes : (m + 1) * lanes] = read(
                starts[1] + m * unit_step, unit_step
            )
        for m in range(2):
            block = read(starts[2] + m * height, height)
            for n in range(height // factor):
                q = 2 * (k * (height // factor) + n) + m
                grad_ref[pl.ds(q, factor, stride=factor), :] = block[n * factor : (n + 1) * factor]
        tall = 2 * factor // chunks
        block = read(starts[3], starts[4] - starts[3])
        for m in range(split):
            twin_ref[k * tall : (k + 1) * tall, m * lanes : (m + 1) * lanes] = block[m * tall : (m + 1) * tall]
        if k == 0:
            extra = read(starts[4], 8)
            for n, ref in enumerate((scale_ref, product_ref)):
                for m in range(split):
                    ref[:, m * lanes : (m + 1) * lanes] = extra[n * split + m : n * split + m + 1]


def call(kernel, outs, scratch, *args, scalars=0, loose=()):
    spaces = [pltpu.SMEM if n < scalars else pl.ANY if n in loose else pltpu.VMEM for n in range(len(args))]
    specs = [pl.BlockSpec(memory_space=space) for space in spaces]
    return pl.pallas_call(
        kernel,
        out_shape=[jax.ShapeDtypeStruct(s, d) for s, d in outs],
        in_specs=specs,
        out_specs=[pl.BlockSpec(memory_space=pltpu.VMEM)] * len(outs),
        scratch_shapes=[pltpu.SemaphoreType.DMA if s is None else pltpu.VMEM(*s) for s in scratch],
        interpret=INTERPRET,
    )(*args)


def exchanged(parts, axis, groups=None):
    return lax.all_to_all(
        parts, axis, split_axis=0, concat_axis=0, axis_index_groups=groups, tiled=True
    )


def copies(own, axis, groups):
    return exchanged(jnp.broadcast_to(own, (len(groups[0]),) + own.shape), axis, groups)


def per_device(
    saved_alignment,
    homolog_existence,
    amino_existence,
    couple_delta_adjoint,
    feedforward_adjoint,
    feedforward_scale,
    expansion_matrix,
    contraction_matrix,
    product_scale_vector,
    twin_operand_matrix,
    couple_projection_matrix,
):
    seqs, res, features = saved_alignment.shape
    units = expansion_matrix.shape[1]
    factor = twin_operand_matrix.shape[1] // 2
    pair_width = couple_projection_matrix.shape[1]
    rows = seqs * res
    row_devices, cols, cores = (lax.axis_size(a) for a in ("row", "col", "sub"))
    shards = cols * cores
    blocks = row_devices // shards
    col_res = couple_delta_adjoint.shape[1]
    all_seqs = seqs * shards
    wide = res * factor
    assert (factor, res, blocks, cores, pair_width) == (32, 32, 2, 2, lanes)
    assert col_res == blocks * res and features == 2 * lanes and units == shards * lanes
    x = saved_alignment.reshape(rows, features)
    scale_in = feedforward_scale.reshape(1, features)
    scale_out = product_scale_vector.reshape(1, features)
    twin = twin_operand_matrix.T
    record = wide + lanes
    (keep, right, left, normed_in, hidden, slope, hat_in, hat_out, normed_out, spread) = call(
        forward_kernel,
        [
            ((seqs, lanes), f32),
            ((row_devices // 2, seqs, record), bf16),
            ((shards, seqs, record), bf16),
            ((rows, features), bf16),
            ((rows, units), bf16),
            ((rows, units), f32),
            ((rows, features), f32),
            ((rows, features), f32),
            ((rows, features), bf16),
            ((rows, lanes), f32),
        ],
        [((rows, lanes), f32), ((seqs * factor, lanes), f32)],
        x, homolog_existence, amino_existence.reshape(1, res), scale_in, expansion_matrix,
        contraction_matrix, scale_out, twin,
    )
    alike = [list(range(b, row_devices, 2)) for b in range(2)]
    swap_rows = [(i, i ^ 1) for i in range(row_devices)]
    parity = (lax.axis_index("row") % 2).reshape(1)
    right = exchanged(right, "row", alike)
    records = exchanged(
        jnp.concatenate([right, left], axis=2), ("col", "sub")
    )
    other = lax.ppermute(records[:, :, :record], "row", swap_rows)
    pairs = lanes // col_res
    sets = factor // pairs
    own, send, left, result_adjoint = call(
        pair_kernel,
        [
            ((shards, seqs, wide), bf16),
            ((shards, seqs, wide), bf16),
            ((shards, seqs, wide), bf16),
            ((sets * factor, pairs * lanes), f32),
        ],
        [
            ((all_seqs, wide), bf16),
            ((all_seqs, col_res * factor), bf16),
            ((sets * factor, res * lanes), bf16),
            ((res * lanes, pairs * lanes), bf16),
            ((res * factor, sets * lanes), bf16),
            ((factor * factor, lanes), f32),
            ((sets * factor, pairs * lanes), bf16),
            ((shards, seqs, record), bf16),
            None,
        ],
        parity, records, other, couple_delta_adjoint, couple_projection_matrix,
        scalars=1, loose=(2,),
    )
    own = (own.astype(f32) + lax.ppermute(send, "row", swap_rows).astype(f32)).astype(bf16)
    back = exchanged(jnp.concatenate([own, left], axis=2), ("col", "sub"))
    right_back = exchanged(back[:, :, :wide], "row", alike)
    core = lax.axis_index("sub").reshape(1)
    starts = chunk_rows(rows, features, units, factor, pair_width, shards)
    lines = -(-(starts[4] + 8) // (2 * row_devices)) * 2 * row_devices
    start_adjoint, own, send = call(
        backward_kernel,
        [
            ((rows, features), bf16),
            ((cols, lines, lanes), bf16),
            ((cols, lines, lanes), bf16),
        ],
        [
            ((rows, lanes), f32),
            ((seqs * factor, lanes), f32),
            ((cores, cols, lines, lanes), bf16),
            ((shards, seqs, wide), bf16),
            None,
        ],
        core, back, right_back, keep, feedforward_adjoint.reshape(rows, features), scale_in,
        expansion_matrix, contraction_matrix, scale_out, twin, result_adjoint, normed_in, hidden, slope,
        hat_in, hat_out, normed_out, spread,
        scalars=1, loose=(2,),
    )
    swap = [(0, 1), (1, 0)]
    half = (own.astype(f32) + lax.ppermute(send, "sub", swap).astype(f32)).astype(bf16)
    near = [
        [(2 * m + b) * cols + c for c in range(cols) for b in range(2)] for m in range(row_devices // 2)
    ]
    half = exchanged(half.reshape(2 * cols, lines // 2, lanes), ("row", "col"), near)
    half = half.astype(f32).sum(axis=0).astype(bf16)
    half = exchanged(half.reshape(row_devices // 2, -1, 2, lanes), "row", alike)
    half = half.astype(f32).sum(axis=0).astype(bf16)
    half = copies(half, "row", alike).reshape(lines // 2, lanes)
    half = copies(half, ("row", "col"), near).reshape(cols, lines, lanes)
    other = lax.ppermute(half, "sub", swap)
    grads = call(
        final_kernel,
        [
            ((factor * factor, pair_width), f32),
            ((2 * factor, features), f32),
            ((features, units), f32),
            ((units, features), f32),
            ((1, features), f32),
            ((1, features), f32),
        ],
        [((cols, lines, lanes), bf16), None],
        core, half, other,
        scalars=1, loose=(2,),
    )
    return (
        start_adjoint.reshape(seqs, res, features),
        grads[0],
        grads[1].T,
        grads[2],
        grads[3],
        grads[4].reshape(features),
        grads[5].reshape(features),
    )


def solution(mesh):
    return jax.shard_map(
        per_device,
        mesh=mesh,
        in_specs=(
            P(("col", "sub"), ("groups", "row"), None),
            P(("col", "sub"), ("groups", "row")),
            P(("groups", "row")),
            P(("groups", "row"), ("col", "sub"), None),
            P(("col", "sub"), ("groups", "row"), None),
            P(),
            P(),
            P(),
            P(),
            P(),
            P(),
        ),
        out_specs=(
            P(("col", "sub"), ("groups", "row"), None),
            P("groups", None),
            P("groups", None),
            P("groups", None),
            P("groups", None),
            P("groups"),
            P("groups"),
        ),
        check_vma=False,
    )
```

```python
import math

import jax
import jax.numpy as jnp
from jax import lax
from jax.experimental import pallas as pl
from jax.experimental.pallas import tpu as pltpu
from jax.sharding import PartitionSpec as P

epsilon = 1e-05
lanes = 128
f32 = jnp.float32
bf16 = jnp.bfloat16
INTERPRET = False


def layer_normalize(values):
    centre = jnp.mean(values, axis=-1, keepdims=True)
    centred = values - centre
    variance = jnp.mean(centred * centred, axis=-1, keepdims=True)
    inv_std = lax.rsqrt(variance + epsilon)
    return (centred * inv_std, inv_std)


def standardizer_adjoint(grad_hat, normed, inv_std):
    first_mean = jnp.mean(grad_hat, axis=-1, keepdims=True)
    second_mean = jnp.mean(grad_hat * normed, axis=-1, keepdims=True)
    return inv_std * (grad_hat - first_mean - normed * second_mean)


def plain(a, b):
    return lax.dot_general(a, b, (((1,), (0,)), ((), ())), preferred_element_type=f32)


def last_last(a, b):
    return lax.dot_general(a, b, (((1,), (1,)), ((), ())), preferred_element_type=f32)


def first_first(a, b):
    return lax.dot_general(a, b, (((0,), (0,)), ((), ())), preferred_element_type=f32)


def turn(values, shift):
    shift = shift % lanes
    return values if shift == 0 else pltpu.roll(values, shift, 1)


def lane_index(shape):
    return lax.broadcasted_iota(jnp.int32, shape, 1)


def keep_column(keep, seqs, res):
    rows = seqs * res
    wide = jnp.broadcast_to(keep[:, None, :], (seqs, res, lanes)).reshape(rows, lanes)
    residue = lax.broadcasted_iota(jnp.int32, (rows, lanes), 0) % res
    own = lane_index((rows, lanes)) == residue
    return jnp.sum(jnp.where(own, wide, 0.0), axis=1, keepdims=True)


def fetch(pairs):
    started = [pltpu.make_async_copy(*pair) for pair in pairs]
    for copy in started:
        copy.start()
    return started


def transition(x, scale_in, w_in_ref, scale_out, w_mid_ref, w_in_copy, w_mid_copy, with_slope):
    hat_in, inv_in = layer_normalize(x)
    normed_in = (hat_in * scale_in).astype(bf16)
    w_in_copy.wait()
    pre = plain(normed_in, w_in_ref[...])
    share = 0.5 * (1.0 + lax.erf(pre * math.sqrt(0.5)))
    hidden = (pre * share).astype(bf16)
    slope = None
    if with_slope:
        slope = share + pre * (jnp.exp(-0.5 * pre * pre) * (1.0 / math.sqrt(2.0 * math.pi)))
    w_mid_copy.wait()
    mixed = x + plain(hidden, w_mid_ref[...])
    hat_out, inv_out = layer_normalize(mixed)
    normed_out = (hat_out * scale_out).astype(bf16)
    return normed_in, hidden, slope, hat_in, inv_in, hat_out, inv_out, normed_out


def forward_kernel(
    x_ref, present_ref, residue_ref, scale_in_ref, w_in_hbm, w_mid_hbm, scale_out_ref, twin_ref,
    keep_ref, right_ref, left_ref, left_rows, right_rows, w_in_ref, w_mid_ref, sem_a, sem_b,
):
    copy_in, copy_mid = fetch([(w_in_hbm, w_in_ref, sem_a), (w_mid_hbm, w_mid_ref, sem_b)])
    seqs, res = present_ref.shape
    rows = x_ref.shape[0]
    keep_ref[...] = jnp.zeros((seqs, lanes), f32)
    keep_ref[:, :res] = (present_ref[...] * residue_ref[...]).astype(f32)
    factor = twin_ref.shape[0] // 2
    group = lanes // factor
    normed_out = transition(
        x_ref[...].astype(f32), scale_in_ref[...], w_in_ref, scale_out_ref[...], w_mid_ref, copy_in, copy_mid,
        False,
    )[-1]
    lane = lane_index((rows, lanes))
    keep = keep_ref[...]
    twin = twin_ref[...]
    projected = last_last(
        normed_out, jnp.concatenate([twin, jnp.zeros((lanes - 2 * factor, twin.shape[1]), bf16)], axis=0)
    )
    left_rows[...] = jnp.where(lane < factor, projected * keep_column(keep, seqs, res), 0.0)
    turned = last_last(twin[factor:], normed_out)
    per = lanes // res
    for s in range(seqs):
        tile = turned[:, (s // per) * lanes : (s // per + 1) * lanes]
        right_rows[s * factor : (s + 1) * factor, :] = turn(tile, -(s % per) * res)
    left_pieces = []
    for t in range(res // group):
        tile = left_rows[pl.ds(t * group, seqs, stride=res), :]
        for m in range(1, group):
            tile = tile + turn(left_rows[pl.ds(t * group + m, seqs, stride=res), :], m * factor)
        left_pieces.append(tile)
    left_record = jnp.concatenate(left_pieces + [keep], axis=1).astype(bf16)
    for c in range(left_ref.shape[0]):
        left_ref[c] = left_record
    pieces = []
    for t in range(factor // per):
        tile = right_rows[pl.ds(t * per, seqs, stride=factor), :] * keep
        for m in range(1, per):
            piece = right_rows[pl.ds(t * per + m, seqs, stride=factor), :] * keep
            tile = tile + turn(piece, m * res)
        pieces.append(tile)
    record = jnp.concatenate(pieces + [keep], axis=1).astype(bf16)
    for c in range(right_ref.shape[0]):
        right_ref[c] = record


def pair_kernel(
    parity_ref, rec_ref, other_ref, cot_hbm, proj_ref, back_ref, send_ref, grad_ref,
    left_all, right_all, outer_all, adjoint_all, pulled_all, proj_rows, proj_all, other_all, cot_ref, sem, sem_b,
):
    shards, seqs, record = other_ref.shape
    start, copy_cot = fetch([(other_ref, other_all, sem), (cot_hbm, cot_ref, sem_b)])
    blocks = 2
    even = parity_ref[0] == 0
    all_seqs = shards * seqs
    res = cot_ref.shape[0]
    cols = cot_ref.shape[1]
    wide = send_ref.shape[2]
    factor = wide // res
    pairs = lanes // cols
    sets = factor // pairs
    half = cols // blocks
    lane = lane_index((all_seqs, lanes))

    def left_tile(t):
        at = record + t * lanes
        return rec_ref[:, :, at : at + lanes].astype(f32).reshape(all_seqs, lanes)

    def right_tiles(t):
        own = rec_ref[:, :, t * lanes : (t + 1) * lanes].astype(f32).reshape(all_seqs, lanes)
        other = other_all[:, :, t * lanes : (t + 1) * lanes].astype(f32).reshape(all_seqs, lanes)
        return jnp.where(even, own, other), jnp.where(even, other, own)

    proj_rows[...] = proj_ref[...].astype(f32)
    for n in range(sets):
        for k in range(pairs):
            proj_all[n * factor : (n + 1) * factor, k * lanes : (k + 1) * lanes] = proj_rows[
                pl.ds(n * pairs + k, factor, stride=factor), :
            ].astype(bf16)
    for t in range(wide // lanes):
        left_all[:, t * lanes : (t + 1) * lanes] = left_tile(t).astype(bf16)
    start.wait()
    for t in range(wide // lanes):
        a, b = right_tiles(t)
        first = jnp.where(
            lane < 32, a, jnp.where(lane < 64, turn(b, 32), jnp.where(lane < 96, turn(a, 32), turn(b, 64)))
        )
        second = jnp.where(
            lane < 32, turn(a, 64), jnp.where(lane < 64, turn(b, 96), jnp.where(lane < 96, turn(a, 96), b))
        )
        right_all[:, 2 * t * lanes : (2 * t + 1) * lanes] = first.astype(bf16)
        right_all[:, (2 * t + 1) * lanes : (2 * t + 2) * lanes] = second.astype(bf16)
    last = wide // lanes
    keep_rows = left_tile(last).astype(bf16)
    a, b = right_tiles(last)
    keep_cols = (a + turn(b, half)).astype(bf16)
    count = first_first(keep_cols, keep_rows)[:cols]
    inverse = 1.0 / jnp.maximum(count, 1.0)
    nothing = jnp.zeros((cols, lanes), bf16)
    copy_cot.wait()
    for i in range(res):
        scaled = (cot_ref[i].astype(f32) * inverse[:, i : i + 1]).astype(bf16)
        at = i * lanes
        for k in range(pairs):
            for m in range(pairs):
                adjoint_all[at + k * cols : at + (k + 1) * cols, m * lanes : (m + 1) * lanes] = (
                    scaled if k == m else nothing
                )
    step = 256 // factor
    for c in range(res // step):
        outer = first_first(left_all[:, c * step * factor : (c + 1) * step * factor], right_all[...])
        for i in range(step):
            at = (c * step + i) * lanes
            for n in range(sets):
                outer_all[n * factor : (n + 1) * factor, at : at + lanes] = outer[
                    i * factor : (i + 1) * factor, n * lanes : (n + 1) * lanes
                ].astype(bf16)
        pulled = last_last(proj_all[...], adjoint_all[c * step * lanes : (c + 1) * step * lanes, :])
        for i in range(step):
            at = (c * step + i) * factor
            for n in range(sets):
                pulled_all[at : at + factor, n * lanes : (n + 1) * lanes] = pulled[
                    n * factor : (n + 1) * factor, i * lanes : (i + 1) * lanes
                ].astype(bf16)
    grad_ref[...] = plain(outer_all[...], adjoint_all[...]).astype(bf16)
    grad_left = last_last(right_all[...], pulled_all[...])
    grad_right = plain(left_all[...], pulled_all[...])

    def put(ref, at, values):
        ref[:, :, at : at + lanes] = values.reshape(shards, seqs, lanes).astype(bf16)

    for t in range(wide // lanes):
        put(back_ref, wide + t * lanes, grad_left[:, t * lanes : (t + 1) * lanes])
        a = grad_right[:, 2 * t * lanes : (2 * t + 1) * lanes]
        b = grad_right[:, (2 * t + 1) * lanes : (2 * t + 2) * lanes]
        first = jnp.where(
            lane < 32, a, jnp.where(lane < 64, turn(a, 96), jnp.where(lane < 96, turn(b, 64), turn(b, 32)))
        )
        second = jnp.where(
            lane < 32, turn(a, 96), jnp.where(lane < 64, turn(a, 64), jnp.where(lane < 96, turn(b, 32), b))
        )
        put(back_ref, t * lanes, jnp.where(even, first, second))
        put(send_ref, t * lanes, jnp.where(even, second, first))


def chunk_rows(rows, features, hidden, factor, pair_width, chunks):
    sizes = (
        features * hidden // chunks // lanes,
        hidden * features // chunks // lanes,
        factor * factor * pair_width // chunks // lanes,
        2 * factor * features // chunks // lanes,
    )
    starts = [0]
    for size in sizes:
        starts.append(starts[-1] + size)
    return starts


def backward_kernel(
    core_ref, left_hbm, right_hbm, keep_ref, x_ref, cot_ref, scale_in_ref, w_in_hbm, w_mid_hbm,
    scale_out_ref, twin_ref, grad_hbm, out_ref, own_ref, send_ref,
    left_rows, right_rows, chunks_ref, left_ref, right_all, w_in_ref, w_mid_ref, grad_ref,
    sem_a, sem_b, sem_c, sem_d, sem_e,
):
    copy_in, copy_mid, copy_left, copy_right, copy_grad = fetch([
        (w_in_hbm, w_in_ref, sem_a), (w_mid_hbm, w_mid_ref, sem_b), (left_hbm, left_ref, sem_c),
        (right_hbm, right_all, sem_d), (grad_hbm, grad_ref, sem_e),
    ])
    seqs = keep_ref.shape[0]
    rows, features = cot_ref.shape
    res = rows // seqs
    factor = twin_ref.shape[0] // 2
    group = lanes // factor
    per = lanes // res
    cols = own_ref.shape[0]
    chunks = 2 * cols
    units = w_in_ref.shape[1]
    pair_width = lanes
    starts = chunk_rows(rows, features, units, factor, pair_width, chunks)
    keep = keep_ref[...]
    lane_small = lane_index((seqs, lanes))
    normed_in, hidden, slope, hat_in, inv_in, hat_out, inv_out, normed_out = transition(
        x_ref[...].astype(f32), scale_in_ref[...], w_in_ref, scale_out_ref[...], w_mid_ref, copy_in, copy_mid,
        True,
    )
    copy_left.wait()
    half = res * factor
    for t in range(res // group):
        tile = jnp.sum(left_ref[:, :, half + t * lanes : half + (t + 1) * lanes].astype(f32), axis=0)
        for m in range(group):
            piece = jnp.where(lane_small < factor, turn(tile, -m * factor), 0.0)
            left_rows[pl.ds(t * group + m, seqs, stride=res), :] = piece
    copy_right.wait()
    for t in range(factor // per):
        tile = jnp.sum(right_all[:, :, t * lanes : (t + 1) * lanes].astype(f32), axis=0)
        for m in range(per):
            right_rows[pl.ds(t * per + m, seqs, stride=factor), :] = turn(tile, -m * res) * keep
    tiles = []
    for h in range(rows // lanes):
        tile = right_rows[h * per * factor : (h * per + 1) * factor, :]
        for m in range(1, per):
            at = (h * per + m) * factor
            tile = tile + turn(right_rows[at : at + factor, :], m * res)
        tiles.append(tile)
    turned = jnp.concatenate(tiles, axis=1)
    turned = jnp.concatenate(
        [jnp.zeros((factor, rows), f32), turned, jnp.zeros((lanes - 2 * factor, rows), f32)], axis=0
    )
    grad_proj = (left_rows[...] * keep_column(keep, seqs, res) + jnp.transpose(turned)).astype(bf16)
    twin = twin_ref[...]
    twin = jnp.concatenate([twin, jnp.zeros((lanes - 2 * factor, features), bf16)], axis=0)
    operand_adjoint = first_first(grad_proj, normed_out)
    rescaled = plain(grad_proj, twin)
    product_adjoint = jnp.sum(rescaled * hat_out, axis=0, keepdims=True)
    combined = cot_ref[...].astype(f32) + standardizer_adjoint(
        rescaled * scale_out_ref[...], hat_out, inv_out
    )
    mixed_half = combined.astype(bf16)
    grad_hidden = last_last(mixed_half, w_mid_ref[...])
    grad_pre = (slope * grad_hidden).astype(bf16)
    grad_in = last_last(grad_pre, w_in_ref[...])
    scale_adjoint = jnp.sum(grad_in * hat_in, axis=0, keepdims=True)
    out_ref[...] = (
        combined + standardizer_adjoint(grad_in * scale_in_ref[...], hat_in, inv_in)
    ).astype(bf16)
    hidden_adjoint = first_first(hidden, mixed_half)
    expansion_adjoint = first_first(normed_in, grad_pre)
    split = features // lanes
    copy_grad.wait()

    def put(k, at, values):
        chunks_ref[k // cols, k % cols, at : at + values.shape[0], :] = values.astype(bf16)

    unit_step = units // chunks
    for k in range(chunks):
        put(k, starts[0], expansion_adjoint[:, k * unit_step : (k + 1) * unit_step])
        for m in range(split):
            put(k, starts[1] + m * unit_step,
                hidden_adjoint[k * unit_step : (k + 1) * unit_step, m * lanes : (m + 1) * lanes])
        height = grad_ref.shape[0] // chunks
        for m in range(grad_ref.shape[1] // lanes):
            put(k, starts[2] + m * height, grad_ref[k * height : (k + 1) * height, m * lanes : (m + 1) * lanes])
        height = 2 * factor // chunks
        tail = [
            operand_adjoint[k * height : (k + 1) * height, m * lanes : (m + 1) * lanes] for m in range(split)
        ]
        row = lax.broadcasted_iota(jnp.int32, (8, lanes), 0)
        extra = jnp.zeros((8, lanes), f32)
        if k == 0:
            for n, vector in enumerate((scale_adjoint, product_adjoint)):
                for m in range(split):
                    extra = jnp.where(row == n * split + m, vector[:, m * lanes : (m + 1) * lanes], extra)
        rest = chunks_ref.shape[2] - starts[4] - 8
        block = jnp.concatenate(tail + [extra, jnp.zeros((rest, lanes), f32)], axis=0)
        put(k, starts[3], block)
    core = core_ref[0]
    own_ref[...] = chunks_ref[core]
    send_ref[...] = chunks_ref[1 - core]


def final_kernel(
    core_ref, half_ref, other_ref, grad_hbm, twin_ref, w_in_hbm, w_mid_hbm, scale_ref, product_ref,
    grad_ref, w_in_ref, w_mid_ref, sem_grad, sem_in, sem_mid,
):
    cols = half_ref.shape[0]
    chunks = 2 * cols
    features, units = w_in_ref.shape
    factor = twin_ref.shape[0] // 2
    starts = chunk_rows(0, features, units, factor, lanes, chunks)
    split = features // lanes
    unit_step = units // chunks
    core = core_ref[0]
    height = factor * factor // 2 // chunks

    def read(k, at, size):
        return jnp.where(
            core == k // cols,
            half_ref[k % cols, at : at + size, :].astype(f32),
            other_ref[k % cols, at : at + size, :].astype(f32),
        )

    leaving = []
    for k in range(chunks):
        span = slice(k * unit_step, (k + 1) * unit_step)
        w_in_ref[:, span] = read(k, starts[0], features)
        leaving.append(pltpu.make_async_copy(w_in_ref.at[:, span], w_in_hbm.at[:, span], sem_in.at[k]))
        leaving[-1].start()
        for m in range(split):
            w_mid_ref[span, m * lanes : (m + 1) * lanes] = read(k, starts[1] + m * unit_step, unit_step)
        leaving.append(pltpu.make_async_copy(w_mid_ref.at[span, :], w_mid_hbm.at[span, :], sem_mid.at[k]))
        leaving[-1].start()
    for k in range(chunks):
        for m in range(2):
            block = read(k, starts[2] + m * height, height)
            for n in range(height // factor):
                q = 2 * (k * (height // factor) + n) + m
                grad_ref[pl.ds(q, factor, stride=factor), :] = block[n * factor : (n + 1) * factor]
    leaving.append(pltpu.make_async_copy(grad_ref, grad_hbm, sem_grad))
    leaving[-1].start()
    tall = 2 * factor // chunks
    for k in range(chunks):
        block = read(k, starts[3], starts[4] - starts[3])
        for m in range(split):
            twin_ref[k * tall : (k + 1) * tall, m * lanes : (m + 1) * lanes] = block[m * tall : (m + 1) * tall]
    extra = read(0, starts[4], 8)
    for n, ref in enumerate((scale_ref, product_ref)):
        for m in range(split):
            ref[:, m * lanes : (m + 1) * lanes] = extra[n * split + m : n * split + m + 1]
    for copy in leaving:
        copy.wait()


def call(kernel, outs, scratch, *args, scalars=0, loose=(), loose_outs=()):
    spaces = [pltpu.SMEM if n < scalars else pl.ANY if n in loose else pltpu.VMEM for n in range(len(args))]
    specs = [pl.BlockSpec(memory_space=space) for space in spaces]
    return pl.pallas_call(
        kernel,
        out_shape=[jax.ShapeDtypeStruct(s, d) for s, d in outs],
        in_specs=specs,
        out_specs=[
            pl.BlockSpec(memory_space=pl.ANY if n in loose_outs else pltpu.VMEM) for n in range(len(outs))
        ],
        scratch_shapes=[
            pltpu.SemaphoreType.DMA if s is None
            else pltpu.SemaphoreType.DMA(s) if isinstance(s[0], int)
            else pltpu.VMEM(*s)
            for s in scratch
        ],
        interpret=INTERPRET,
    )(*args)


def exchanged(parts, axis, groups=None):
    return lax.all_to_all(
        parts, axis, split_axis=0, concat_axis=0, axis_index_groups=groups, tiled=True
    )


def copies(own, axis, groups):
    return exchanged(jnp.broadcast_to(own, (len(groups[0]),) + own.shape), axis, groups)


def per_device(
    saved_alignment,
    homolog_existence,
    amino_existence,
    couple_delta_adjoint,
    feedforward_adjoint,
    feedforward_scale,
    expansion_matrix,
    contraction_matrix,
    product_scale_vector,
    twin_operand_matrix,
    couple_projection_matrix,
):
    seqs, res, features = saved_alignment.shape
    units = expansion_matrix.shape[1]
    factor = twin_operand_matrix.shape[1] // 2
    pair_width = couple_projection_matrix.shape[1]
    rows = seqs * res
    row_devices, cols, cores = (lax.axis_size(a) for a in ("row", "col", "sub"))
    shards = cols * cores
    blocks = row_devices // shards
    col_res = couple_delta_adjoint.shape[1]
    all_seqs = seqs * shards
    wide = res * factor
    assert (factor, res, blocks, cores, pair_width) == (32, 32, 2, 2, lanes)
    assert col_res == blocks * res and features == 2 * lanes and units == shards * lanes
    x = saved_alignment.reshape(rows, features)
    scale_in = feedforward_scale.reshape(1, features)
    scale_out = product_scale_vector.reshape(1, features)
    twin = twin_operand_matrix.T
    record = wide + lanes
    keep, right, left = call(
        forward_kernel,
        [
            ((seqs, lanes), f32),
            ((row_devices // 2, seqs, record), bf16),
            ((shards, seqs, record), bf16),
        ],
        [
            ((rows, lanes), f32),
            ((seqs * factor, lanes), f32),
            ((features, units), bf16),
            ((units, features), bf16),
            None,
            None,
        ],
        x, homolog_existence, amino_existence.reshape(1, res), scale_in, expansion_matrix,
        contraction_matrix, scale_out, twin,
        loose=(4, 5),
    )
    alike = [list(range(b, row_devices, 2)) for b in range(2)]
    swap_rows = [(i, i ^ 1) for i in range(row_devices)]
    parity = (lax.axis_index("row") % 2).reshape(1)
    right = exchanged(right, "row", alike)
    records = exchanged(
        jnp.concatenate([right, left], axis=2), ("col", "sub")
    )
    other = lax.ppermute(records[:, :, :record], "row", swap_rows)
    pairs = lanes // col_res
    sets = factor // pairs
    back, send, result_adjoint = call(
        pair_kernel,
        [
            ((shards, seqs, 2 * wide), bf16),
            ((shards, seqs, wide), bf16),
            ((sets * factor, pairs * lanes), bf16),
        ],
        [
            ((all_seqs, wide), bf16),
            ((all_seqs, col_res * factor), bf16),
            ((sets * factor, res * lanes), bf16),
            ((res * lanes, pairs * lanes), bf16),
            ((res * factor, sets * lanes), bf16),
            ((factor * factor, lanes), f32),
            ((sets * factor, pairs * lanes), bf16),
            ((shards, seqs, record), bf16),
            ((res, col_res, lanes), bf16),
            None,
            None,
        ],
        parity, records, other, couple_delta_adjoint, couple_projection_matrix,
        scalars=1, loose=(2, 3),
    )
    paired = jnp.pad(lax.ppermute(send, "row", swap_rows), ((0, 0), (0, 0), (0, wide)))
    back = exchanged((back.astype(f32) + paired.astype(f32)).astype(bf16), ("col", "sub"))
    right_back = exchanged(back[:, :, :wide], "row", alike)
    core = lax.axis_index("sub").reshape(1)
    starts = chunk_rows(rows, features, units, factor, pair_width, shards)
    lines = -(-(starts[4] + 8) // (2 * row_devices)) * 2 * row_devices
    start_adjoint, own, send = call(
        backward_kernel,
        [
            ((rows, features), bf16),
            ((cols, lines, lanes), bf16),
            ((cols, lines, lanes), bf16),
        ],
        [
            ((rows, lanes), f32),
            ((seqs * factor, lanes), f32),
            ((cores, cols, lines, lanes), bf16),
            ((shards, seqs, 2 * wide), bf16),
            ((shards, seqs, wide), bf16),
            ((features, units), bf16),
            ((units, features), bf16),
            ((sets * factor, pairs * lanes), bf16),
            None,
            None,
            None,
            None,
            None,
        ],
        core, back, right_back, keep, x, feedforward_adjoint.reshape(rows, features), scale_in,
        expansion_matrix, contraction_matrix, scale_out, twin, result_adjoint,
        scalars=1, loose=(1, 2, 7, 8, 11),
    )
    swap = [(0, 1), (1, 0)]
    half = (own.astype(f32) + lax.ppermute(send, "sub", swap).astype(f32)).astype(bf16)
    near = [
        [(2 * m + b) * cols + c for c in range(cols) for b in range(2)] for m in range(row_devices // 2)
    ]
    half = exchanged(half.reshape(2 * cols, lines // 2, lanes), ("row", "col"), near)
    half = half.astype(f32).sum(axis=0).astype(bf16)
    half = exchanged(half.reshape(row_devices // 2, -1, 2, lanes), "row", alike)
    half = half.astype(f32).sum(axis=0).astype(bf16)
    half = copies(half, "row", alike).reshape(lines // 2, lanes)
    half = copies(half, ("row", "col"), near).reshape(cols, lines, lanes)
    other = lax.ppermute(half, "sub", swap)
    grads = call(
        final_kernel,
        [
            ((factor * factor, pair_width), f32),
            ((2 * factor, features), f32),
            ((features, units), f32),
            ((units, features), f32),
            ((1, features), f32),
            ((1, features), f32),
        ],
        [
            ((factor * factor, pair_width), f32),
            ((features, units), f32),
            ((units, features), f32),
            None,
            (shards,),
            (shards,),
        ],
        core, half, other,
        scalars=1, loose_outs=(0, 2, 3),
    )
    return (
        start_adjoint.reshape(seqs, res, features),
        grads[0],
        grads[1].T,
        grads[2],
        grads[3],
        grads[4].reshape(features),
        grads[5].reshape(features),
    )


def solution(mesh):
    return jax.shard_map(
        per_device,
        mesh=mesh,
        in_specs=(
            P(("col", "sub"), ("groups", "row"), None),
            P(("col", "sub"), ("groups", "row")),
            P(("groups", "row")),
            P(("groups", "row"), ("col", "sub"), None),
            P(("col", "sub"), ("groups", "row"), None),
            P(),
            P(),
            P(),
            P(),
            P(),
            P(),
        ),
        out_specs=(
            P(("col", "sub"), ("groups", "row"), None),
            P("groups", None),
            P("groups", None),
            P("groups", None),
            P("groups", None),
            P("groups"),
            P("groups"),
        ),
        check_vma=False,
    )
```

```python
import math

import jax
import jax.numpy as jnp
from jax import lax
from jax.experimental import pallas as pl
from jax.experimental.pallas import tpu as pltpu
from jax.sharding import PartitionSpec as P

epsilon = 1e-05
lanes = 128
f32 = jnp.float32
bf16 = jnp.bfloat16
INTERPRET = False


def layer_normalize(values):
    centre = jnp.mean(values, axis=-1, keepdims=True)
    centred = values - centre
    variance = jnp.mean(centred * centred, axis=-1, keepdims=True)
    inv_std = lax.rsqrt(variance + epsilon)
    return (centred * inv_std, inv_std)


def standardizer_adjoint(grad_hat, normed, inv_std):
    first_mean = jnp.mean(grad_hat, axis=-1, keepdims=True)
    second_mean = jnp.mean(grad_hat * normed, axis=-1, keepdims=True)
    return inv_std * (grad_hat - first_mean - normed * second_mean)


def plain(a, b):
    return lax.dot_general(a, b, (((1,), (0,)), ((), ())), preferred_element_type=f32)


def last_last(a, b):
    return lax.dot_general(a, b, (((1,), (1,)), ((), ())), preferred_element_type=f32)


def first_first(a, b):
    return lax.dot_general(a, b, (((0,), (0,)), ((), ())), preferred_element_type=f32)


def turn(values, shift):
    shift = shift % lanes
    return values if shift == 0 else pltpu.roll(values, shift, 1)


def lane_index(shape):
    return lax.broadcasted_iota(jnp.int32, shape, 1)


def keep_column(keep, seqs, res):
    rows = seqs * res
    wide = jnp.broadcast_to(keep[:, None, :], (seqs, res, lanes)).reshape(rows, lanes)
    residue = lax.broadcasted_iota(jnp.int32, (rows, lanes), 0) % res
    own = lane_index((rows, lanes)) == residue
    return jnp.sum(jnp.where(own, wide, 0.0), axis=1, keepdims=True)


def transition(x, scale_in, w_in_ref, scale_out, w_mid_ref, with_slope):
    hat_in, inv_in = layer_normalize(x)
    normed_in = (hat_in * scale_in).astype(bf16)
    pre = plain(normed_in, w_in_ref[...])
    share = 0.5 * (1.0 + lax.erf(pre * math.sqrt(0.5)))
    hidden = (pre * share).astype(bf16)
    slope = None
    if with_slope:
        slope = share + pre * (jnp.exp(-0.5 * pre * pre) * (1.0 / math.sqrt(2.0 * math.pi)))
    mixed = x + plain(hidden, w_mid_ref[...])
    hat_out, inv_out = layer_normalize(mixed)
    normed_out = (hat_out * scale_out).astype(bf16)
    return normed_in, hidden, slope, hat_in, inv_in, hat_out, inv_out, normed_out


def forward_kernel(
    x_ref, present_ref, residue_ref, scale_in_ref, w_in_ref, w_mid_ref, scale_out_ref, twin_ref,
    keep_ref, right_ref, left_ref, left_rows, right_rows,
):
    seqs, res = present_ref.shape
    rows = x_ref.shape[0]
    keep_ref[...] = jnp.zeros((seqs, lanes), f32)
    keep_ref[:, :res] = (present_ref[...] * residue_ref[...]).astype(f32)
    factor = twin_ref.shape[0] // 2
    group = lanes // factor
    normed_out = transition(
        x_ref[...].astype(f32), scale_in_ref[...], w_in_ref, scale_out_ref[...], w_mid_ref, False,
    )[-1]
    lane = lane_index((rows, lanes))
    keep = keep_ref[...]
    twin = twin_ref[...]
    projected = last_last(
        normed_out, jnp.concatenate([twin, jnp.zeros((lanes - 2 * factor, twin.shape[1]), bf16)], axis=0)
    )
    left_rows[...] = jnp.where(lane < factor, projected * keep_column(keep, seqs, res), 0.0)
    turned = last_last(twin[factor:], normed_out)
    per = lanes // res
    for s in range(seqs):
        tile = turned[:, (s // per) * lanes : (s // per + 1) * lanes]
        right_rows[s * factor : (s + 1) * factor, :] = turn(tile, -(s % per) * res)
    left_pieces = []
    for t in range(res // group):
        tile = left_rows[pl.ds(t * group, seqs, stride=res), :]
        for m in range(1, group):
            tile = tile + turn(left_rows[pl.ds(t * group + m, seqs, stride=res), :], m * factor)
        left_pieces.append(tile)
    left_record = jnp.concatenate(left_pieces + [keep], axis=1).astype(bf16)
    for c in range(left_ref.shape[0]):
        left_ref[c] = left_record
    pieces = []
    for t in range(factor // per):
        tile = right_rows[pl.ds(t * per, seqs, stride=factor), :] * keep
        for m in range(1, per):
            piece = right_rows[pl.ds(t * per + m, seqs, stride=factor), :] * keep
            tile = tile + turn(piece, m * res)
        pieces.append(tile)
    record = jnp.concatenate(pieces + [keep], axis=1).astype(bf16)
    for c in range(right_ref.shape[0]):
        right_ref[c] = record


def pair_kernel(
    parity_ref, rec_ref, other_ref, cot_ref, proj_ref, back_ref, send_ref, grad_ref,
    left_all, right_all, outer_all, adjoint_all, pulled_all, proj_rows, proj_all,
):
    shards, seqs, record = other_ref.shape
    blocks = 2
    even = parity_ref[0] == 0
    all_seqs = shards * seqs
    res = cot_ref.shape[0]
    cols = cot_ref.shape[1]
    wide = send_ref.shape[2]
    factor = wide // res
    pairs = lanes // cols
    sets = factor // pairs
    half = cols // blocks
    lane = lane_index((all_seqs, lanes))

    def left_tile(t):
        at = record + t * lanes
        return rec_ref[:, :, at : at + lanes].astype(f32).reshape(all_seqs, lanes)

    def right_tiles(t):
        own = rec_ref[:, :, t * lanes : (t + 1) * lanes].astype(f32).reshape(all_seqs, lanes)
        other = other_ref[:, :, t * lanes : (t + 1) * lanes].astype(f32).reshape(all_seqs, lanes)
        return jnp.where(even, own, other), jnp.where(even, other, own)

    proj_rows[...] = proj_ref[...].astype(f32)
    for n in range(sets):
        for k in range(pairs):
            proj_all[n * factor : (n + 1) * factor, k * lanes : (k + 1) * lanes] = proj_rows[
                pl.ds(n * pairs + k, factor, stride=factor), :
            ].astype(bf16)
    for t in range(wide // lanes):
        left_all[:, t * lanes : (t + 1) * lanes] = left_tile(t).astype(bf16)
    for t in range(wide // lanes):
        a, b = right_tiles(t)
        first = jnp.where(
            lane < 32, a, jnp.where(lane < 64, turn(b, 32), jnp.where(lane < 96, turn(a, 32), turn(b, 64)))
        )
        second = jnp.where(
            lane < 32, turn(a, 64), jnp.where(lane < 64, turn(b, 96), jnp.where(lane < 96, turn(a, 96), b))
        )
        right_all[:, 2 * t * lanes : (2 * t + 1) * lanes] = first.astype(bf16)
        right_all[:, (2 * t + 1) * lanes : (2 * t + 2) * lanes] = second.astype(bf16)
    last = wide // lanes
    keep_rows = left_tile(last).astype(bf16)
    a, b = right_tiles(last)
    keep_cols = (a + turn(b, half)).astype(bf16)
    count = first_first(keep_cols, keep_rows)[:cols]
    inverse = 1.0 / jnp.maximum(count, 1.0)
    nothing = jnp.zeros((cols, lanes), bf16)
    for i in range(res):
        scaled = (cot_ref[i].astype(f32) * inverse[:, i : i + 1]).astype(bf16)
        at = i * lanes
        for k in range(pairs):
            for m in range(pairs):
                adjoint_all[at + k * cols : at + (k + 1) * cols, m * lanes : (m + 1) * lanes] = (
                    scaled if k == m else nothing
                )
    step = 256 // factor
    for c in range(res // step):
        outer = first_first(left_all[:, c * step * factor : (c + 1) * step * factor], right_all[...])
        for i in range(step):
            at = (c * step + i) * lanes
            for n in range(sets):
                outer_all[n * factor : (n + 1) * factor, at : at + lanes] = outer[
                    i * factor : (i + 1) * factor, n * lanes : (n + 1) * lanes
                ].astype(bf16)
        pulled = last_last(proj_all[...], adjoint_all[c * step * lanes : (c + 1) * step * lanes, :])
        for i in range(step):
            at = (c * step + i) * factor
            for n in range(sets):
                pulled_all[at : at + factor, n * lanes : (n + 1) * lanes] = pulled[
                    n * factor : (n + 1) * factor, i * lanes : (i + 1) * lanes
                ].astype(bf16)
    grad_ref[...] = plain(outer_all[...], adjoint_all[...]).astype(bf16)
    grad_left = last_last(right_all[...], pulled_all[...])
    grad_right = plain(left_all[...], pulled_all[...])

    def put(ref, at, values):
        ref[:, :, at : at + lanes] = values.reshape(shards, seqs, lanes).astype(bf16)

    for t in range(wide // lanes):
        put(back_ref, wide + t * lanes, grad_left[:, t * lanes : (t + 1) * lanes])
        a = grad_right[:, 2 * t * lanes : (2 * t + 1) * lanes]
        b = grad_right[:, (2 * t + 1) * lanes : (2 * t + 2) * lanes]
        first = jnp.where(
            lane < 32, a, jnp.where(lane < 64, turn(a, 96), jnp.where(lane < 96, turn(b, 64), turn(b, 32)))
        )
        second = jnp.where(
            lane < 32, turn(a, 96), jnp.where(lane < 64, turn(a, 64), jnp.where(lane < 96, turn(b, 32), b))
        )
        put(back_ref, t * lanes, jnp.where(even, first, second))
        put(send_ref, t * lanes, jnp.where(even, second, first))


def chunk_rows(rows, features, hidden, factor, pair_width, chunks):
    sizes = (
        features * hidden // chunks // lanes,
        hidden * features // chunks // lanes,
        factor * factor * pair_width // chunks // lanes,
        2 * factor * features // chunks // lanes,
    )
    starts = [0]
    for size in sizes:
        starts.append(starts[-1] + size)
    return starts


def backward_kernel(
    core_ref, left_ref, right_ref, keep_ref, x_ref, cot_ref, scale_in_ref, w_in_ref, w_mid_ref,
    scale_out_ref, twin_ref, grad_ref, out_ref, own_ref, send_ref, left_rows, right_rows, chunks_ref,
):
    seqs = keep_ref.shape[0]
    rows, features = cot_ref.shape
    res = rows // seqs
    factor = twin_ref.shape[0] // 2
    group = lanes // factor
    per = lanes // res
    cols = own_ref.shape[0]
    chunks = 2 * cols
    units = w_in_ref.shape[1]
    pair_width = lanes
    starts = chunk_rows(rows, features, units, factor, pair_width, chunks)
    keep = keep_ref[...]
    lane_small = lane_index((seqs, lanes))
    normed_in, hidden, slope, hat_in, inv_in, hat_out, inv_out, normed_out = transition(
        x_ref[...].astype(f32), scale_in_ref[...], w_in_ref, scale_out_ref[...], w_mid_ref, True,
    )
    half = res * factor
    for t in range(res // group):
        tile = jnp.sum(left_ref[:, :, half + t * lanes : half + (t + 1) * lanes].astype(f32), axis=0)
        for m in range(group):
            piece = jnp.where(lane_small < factor, turn(tile, -m * factor), 0.0)
            left_rows[pl.ds(t * group + m, seqs, stride=res), :] = piece
    for t in range(factor // per):
        tile = jnp.sum(right_ref[:, :, t * lanes : (t + 1) * lanes].astype(f32), axis=0)
        for m in range(per):
            right_rows[pl.ds(t * per + m, seqs, stride=factor), :] = turn(tile, -m * res) * keep
    tiles = []
    for h in range(rows // lanes):
        tile = right_rows[h * per * factor : (h * per + 1) * factor, :]
        for m in range(1, per):
            at = (h * per + m) * factor
            tile = tile + turn(right_rows[at : at + factor, :], m * res)
        tiles.append(tile)
    turned = jnp.concatenate(tiles, axis=1)
    turned = jnp.concatenate(
        [jnp.zeros((factor, rows), f32), turned, jnp.zeros((lanes - 2 * factor, rows), f32)], axis=0
    )
    grad_proj = (left_rows[...] * keep_column(keep, seqs, res) + jnp.transpose(turned)).astype(bf16)
    twin = twin_ref[...]
    twin = jnp.concatenate([twin, jnp.zeros((lanes - 2 * factor, features), bf16)], axis=0)
    operand_adjoint = first_first(grad_proj, normed_out)
    rescaled = plain(grad_proj, twin)
    product_adjoint = jnp.sum(rescaled * hat_out, axis=0, keepdims=True)
    combined = cot_ref[...].astype(f32) + standardizer_adjoint(
        rescaled * scale_out_ref[...], hat_out, inv_out
    )
    mixed_half = combined.astype(bf16)
    grad_hidden = last_last(mixed_half, w_mid_ref[...])
    grad_pre = (slope * grad_hidden).astype(bf16)
    grad_in = last_last(grad_pre, w_in_ref[...])
    scale_adjoint = jnp.sum(grad_in * hat_in, axis=0, keepdims=True)
    out_ref[...] = (
        combined + standardizer_adjoint(grad_in * scale_in_ref[...], hat_in, inv_in)
    ).astype(bf16)
    hidden_adjoint = first_first(hidden, mixed_half)
    expansion_adjoint = first_first(normed_in, grad_pre)
    split = features // lanes

    def put(k, at, values):
        chunks_ref[k // cols, k % cols, at : at + values.shape[0], :] = values.astype(bf16)

    unit_step = units // chunks
    for k in range(chunks):
        put(k, starts[0], expansion_adjoint[:, k * unit_step : (k + 1) * unit_step])
        for m in range(split):
            put(k, starts[1] + m * unit_step,
                hidden_adjoint[k * unit_step : (k + 1) * unit_step, m * lanes : (m + 1) * lanes])
        height = grad_ref.shape[0] // chunks
        for m in range(grad_ref.shape[1] // lanes):
            put(k, starts[2] + m * height, grad_ref[k * height : (k + 1) * height, m * lanes : (m + 1) * lanes])
        height = 2 * factor // chunks
        tail = [
            operand_adjoint[k * height : (k + 1) * height, m * lanes : (m + 1) * lanes] for m in range(split)
        ]
        row = lax.broadcasted_iota(jnp.int32, (8, lanes), 0)
        extra = jnp.zeros((8, lanes), f32)
        if k == 0:
            for n, vector in enumerate((scale_adjoint, product_adjoint)):
                for m in range(split):
                    extra = jnp.where(row == n * split + m, vector[:, m * lanes : (m + 1) * lanes], extra)
        rest = chunks_ref.shape[2] - starts[4] - 8
        block = jnp.concatenate(tail + [extra, jnp.zeros((rest, lanes), f32)], axis=0)
        put(k, starts[3], block)
    core = core_ref[0]
    own_ref[...] = chunks_ref[core]
    send_ref[...] = chunks_ref[1 - core]


def final_kernel(
    core_ref, half_ref, other_ref, grad_ref, twin_ref, w_in_ref, w_mid_ref, scale_ref, product_ref
):
    cols = half_ref.shape[0]
    chunks = 2 * cols
    features, units = w_in_ref.shape
    factor = twin_ref.shape[0] // 2
    starts = chunk_rows(0, features, units, factor, lanes, chunks)
    split = features // lanes
    unit_step = units // chunks
    core = core_ref[0]
    height = factor * factor // 2 // chunks

    def read(k, at, size):
        return jnp.where(
            core == k // cols,
            half_ref[k % cols, at : at + size, :].astype(f32),
            other_ref[k % cols, at : at + size, :].astype(f32),
        )

    for k in range(chunks):
        span = slice(k * unit_step, (k + 1) * unit_step)
        w_in_ref[:, span] = read(k, starts[0], features)
        for m in range(split):
            w_mid_ref[span, m * lanes : (m + 1) * lanes] = read(k, starts[1] + m * unit_step, unit_step)
    for k in range(chunks):
        for m in range(2):
            block = read(k, starts[2] + m * height, height)
            for n in range(height // factor):
                q = 2 * (k * (height // factor) + n) + m
                grad_ref[pl.ds(q, factor, stride=factor), :] = block[n * factor : (n + 1) * factor]
    tall = 2 * factor // chunks
    for k in range(chunks):
        block = read(k, starts[3], starts[4] - starts[3])
        for m in range(split):
            twin_ref[k * tall : (k + 1) * tall, m * lanes : (m + 1) * lanes] = block[m * tall : (m + 1) * tall]
    extra = read(0, starts[4], 8)
    for n, ref in enumerate((scale_ref, product_ref)):
        for m in range(split):
            ref[:, m * lanes : (m + 1) * lanes] = extra[n * split + m : n * split + m + 1]


def call(kernel, outs, scratch, *args, scalars=0):
    specs = [pl.BlockSpec(memory_space=pltpu.SMEM)] * scalars
    specs += [pl.BlockSpec(memory_space=pltpu.VMEM)] * (len(args) - scalars)
    return pl.pallas_call(
        kernel,
        out_shape=[jax.ShapeDtypeStruct(s, d) for s, d in outs],
        in_specs=specs,
        out_specs=[pl.BlockSpec(memory_space=pltpu.VMEM)] * len(outs),
        scratch_shapes=[pltpu.VMEM(s, d) for s, d in scratch],
        interpret=INTERPRET,
    )(*args)


def exchanged(parts, axis, groups=None):
    return lax.all_to_all(
        parts, axis, split_axis=0, concat_axis=0, axis_index_groups=groups, tiled=True
    )


def copies(own, axis, groups):
    return exchanged(jnp.broadcast_to(own, (len(groups[0]),) + own.shape), axis, groups)


def per_device(
    saved_alignment,
    homolog_existence,
    amino_existence,
    couple_delta_adjoint,
    feedforward_adjoint,
    feedforward_scale,
    expansion_matrix,
    contraction_matrix,
    product_scale_vector,
    twin_operand_matrix,
    couple_projection_matrix,
):
    seqs, res, features = saved_alignment.shape
    units = expansion_matrix.shape[1]
    factor = twin_operand_matrix.shape[1] // 2
    pair_width = couple_projection_matrix.shape[1]
    rows = seqs * res
    row_devices, cols, cores = (lax.axis_size(a) for a in ("row", "col", "sub"))
    shards = cols * cores
    blocks = row_devices // shards
    col_res = couple_delta_adjoint.shape[1]
    all_seqs = seqs * shards
    wide = res * factor
    assert (factor, res, blocks, cores, pair_width) == (32, 32, 2, 2, lanes)
    assert col_res == blocks * res and features == 2 * lanes and units == shards * lanes
    x = saved_alignment.reshape(rows, features)
    scale_in = feedforward_scale.reshape(1, features)
    scale_out = product_scale_vector.reshape(1, features)
    twin = twin_operand_matrix.T
    record = wide + lanes
    keep, right, left = call(
        forward_kernel,
        [
            ((seqs, lanes), f32),
            ((row_devices // 2, seqs, record), bf16),
            ((shards, seqs, record), bf16),
        ],
        [
            ((rows, lanes), f32),
            ((seqs * factor, lanes), f32),
        ],
        x, homolog_existence, amino_existence.reshape(1, res), scale_in, expansion_matrix,
        contraction_matrix, scale_out, twin,
    )
    alike = [list(range(b, row_devices, 2)) for b in range(2)]
    swap_rows = [(i, i ^ 1) for i in range(row_devices)]
    parity = (lax.axis_index("row") % 2).reshape(1)
    right = exchanged(right, "row", alike)
    records = exchanged(
        jnp.concatenate([right, left], axis=2), ("col", "sub")
    )
    other = lax.ppermute(records[:, :, :record], "row", swap_rows)
    pairs = lanes // col_res
    sets = factor // pairs
    back, send, result_adjoint = call(
        pair_kernel,
        [
            ((shards, seqs, 2 * wide), bf16),
            ((shards, seqs, wide), bf16),
            ((sets * factor, pairs * lanes), bf16),
        ],
        [
            ((all_seqs, wide), bf16),
            ((all_seqs, col_res * factor), bf16),
            ((sets * factor, res * lanes), bf16),
            ((res * lanes, pairs * lanes), bf16),
            ((res * factor, sets * lanes), bf16),
            ((factor * factor, lanes), f32),
            ((sets * factor, pairs * lanes), bf16),
        ],
        parity, records, other, couple_delta_adjoint, couple_projection_matrix,
        scalars=1,
    )
    paired = jnp.pad(lax.ppermute(send, "row", swap_rows), ((0, 0), (0, 0), (0, wide)))
    back = exchanged((back.astype(f32) + paired.astype(f32)).astype(bf16), ("col", "sub"))
    right_back = exchanged(back[:, :, :wide], "row", alike)
    core = lax.axis_index("sub").reshape(1)
    starts = chunk_rows(rows, features, units, factor, pair_width, shards)
    lines = -(-(starts[4] + 8) // (2 * row_devices)) * 2 * row_devices
    start_adjoint, own, send = call(
        backward_kernel,
        [
            ((rows, features), bf16),
            ((cols, lines, lanes), bf16),
            ((cols, lines, lanes), bf16),
        ],
        [
            ((rows, lanes), f32),
            ((seqs * factor, lanes), f32),
            ((cores, cols, lines, lanes), bf16),
        ],
        core, back, right_back, keep, x, feedforward_adjoint.reshape(rows, features), scale_in,
        expansion_matrix, contraction_matrix, scale_out, twin, result_adjoint,
        scalars=1,
    )
    swap = [(0, 1), (1, 0)]
    half = (own.astype(f32) + lax.ppermute(send, "sub", swap).astype(f32)).astype(bf16)
    near = [
        [(2 * m + b) * cols + c for c in range(cols) for b in range(2)] for m in range(row_devices // 2)
    ]
    half = exchanged(half.reshape(2 * cols, lines // 2, lanes), ("row", "col"), near)
    half = half.astype(f32).sum(axis=0).astype(bf16)
    half = exchanged(half.reshape(row_devices // 2, -1, 2, lanes), "row", alike)
    half = half.astype(f32).sum(axis=0).astype(bf16)
    half = copies(half, "row", alike).reshape(lines // 2, lanes)
    half = copies(half, ("row", "col"), near).reshape(cols, lines, lanes)
    other = lax.ppermute(half, "sub", swap)
    grads = call(
        final_kernel,
        [
            ((factor * factor, pair_width), f32),
            ((2 * factor, features), f32),
            ((features, units), f32),
            ((units, features), f32),
            ((1, features), f32),
            ((1, features), f32),
        ],
        [],
        core, half, other,
        scalars=1,
    )
    return (
        start_adjoint.reshape(seqs, res, features),
        grads[0],
        grads[1].T,
        grads[2],
        grads[3],
        grads[4].reshape(features),
        grads[5].reshape(features),
    )


def solution(mesh):
    return jax.shard_map(
        per_device,
        mesh=mesh,
        in_specs=(
            P(("col", "sub"), ("groups", "row"), None),
            P(("col", "sub"), ("groups", "row")),
            P(("groups", "row")),
            P(("groups", "row"), ("col", "sub"), None),
            P(("col", "sub"), ("groups", "row"), None),
            P(),
            P(),
            P(),
            P(),
            P(),
            P(),
        ),
        out_specs=(
            P(("col", "sub"), ("groups", "row"), None),
            P("groups", None),
            P("groups", None),
            P("groups", None),
            P("groups", None),
            P("groups"),
            P("groups"),
        ),
        check_vma=False,
    )
```

```python
import math

import jax
import jax.numpy as jnp
from jax import lax
from jax.experimental import pallas as pl
from jax.experimental.pallas import tpu as pltpu
from jax.sharding import PartitionSpec as P

epsilon = 1e-05
lanes = 128
f32 = jnp.float32
bf16 = jnp.bfloat16
INTERPRET = False


def layer_normalize(values):
    centre = jnp.mean(values, axis=-1, keepdims=True)
    centred = values - centre
    variance = jnp.mean(centred * centred, axis=-1, keepdims=True)
    inv_std = lax.rsqrt(variance + epsilon)
    return (centred * inv_std, inv_std)


def standardizer_adjoint(grad_hat, normed, inv_std):
    first_mean = jnp.mean(grad_hat, axis=-1, keepdims=True)
    second_mean = jnp.mean(grad_hat * normed, axis=-1, keepdims=True)
    return inv_std * (grad_hat - first_mean - normed * second_mean)


def plain(a, b):
    return lax.dot_general(a, b, (((1,), (0,)), ((), ())), preferred_element_type=f32)


def last_last(a, b):
    return lax.dot_general(a, b, (((1,), (1,)), ((), ())), preferred_element_type=f32)


def first_first(a, b):
    return lax.dot_general(a, b, (((0,), (0,)), ((), ())), preferred_element_type=f32)


def turn(values, shift):
    shift = shift % lanes
    return values if shift == 0 else pltpu.roll(values, shift, 1)


def lane_index(shape):
    return lax.broadcasted_iota(jnp.int32, shape, 1)


def keep_column(keep, seqs, res):
    rows = seqs * res
    wide = jnp.broadcast_to(keep[:, None, :], (seqs, res, lanes)).reshape(rows, lanes)
    residue = lax.broadcasted_iota(jnp.int32, (rows, lanes), 0) % res
    own = lane_index((rows, lanes)) == residue
    return jnp.sum(jnp.where(own, wide, 0.0), axis=1, keepdims=True)


def transition(x, scale_in, w_in_ref, scale_out, w_mid_ref, with_slope):
    hat_in, inv_in = layer_normalize(x)
    normed_in = (hat_in * scale_in).astype(bf16)
    pre = plain(normed_in, w_in_ref[...])
    share = 0.5 * (1.0 + lax.erf(pre * math.sqrt(0.5)))
    hidden = (pre * share).astype(bf16)
    slope = None
    if with_slope:
        slope = share + pre * (jnp.exp(-0.5 * pre * pre) * (1.0 / math.sqrt(2.0 * math.pi)))
    mixed = x + plain(hidden, w_mid_ref[...])
    hat_out, inv_out = layer_normalize(mixed)
    normed_out = (hat_out * scale_out).astype(bf16)
    return normed_in, hidden, slope, hat_in, inv_in, hat_out, inv_out, normed_out


def forward_kernel(
    x_ref, present_ref, residue_ref, scale_in_ref, w_in_ref, w_mid_ref, scale_out_ref, twin_ref,
    keep_ref, right_ref, left_ref, left_rows, right_rows,
):
    seqs, res = present_ref.shape
    rows = x_ref.shape[0]
    keep_ref[...] = jnp.zeros((seqs, lanes), f32)
    keep_ref[:, :res] = (present_ref[...] * residue_ref[...]).astype(f32)
    factor = twin_ref.shape[0] // 2
    group = lanes // factor
    normed_out = transition(
        x_ref[...].astype(f32), scale_in_ref[...], w_in_ref, scale_out_ref[...], w_mid_ref, False,
    )[-1]
    lane = lane_index((rows, lanes))
    keep = keep_ref[...]
    twin = twin_ref[...]
    projected = last_last(
        normed_out, jnp.concatenate([twin, jnp.zeros((lanes - 2 * factor, twin.shape[1]), bf16)], axis=0)
    )
    left_rows[...] = jnp.where(lane < factor, projected * keep_column(keep, seqs, res), 0.0)
    turned = last_last(twin[factor:], normed_out)
    per = lanes // res
    for s in range(seqs):
        tile = turned[:, (s // per) * lanes : (s // per + 1) * lanes]
        right_rows[s * factor : (s + 1) * factor, :] = turn(tile, -(s % per) * res)
    left_pieces = []
    for t in range(res // group):
        tile = left_rows[pl.ds(t * group, seqs, stride=res), :]
        for m in range(1, group):
            tile = tile + turn(left_rows[pl.ds(t * group + m, seqs, stride=res), :], m * factor)
        left_pieces.append(tile)
    left_record = jnp.concatenate(left_pieces + [keep], axis=1).astype(bf16)
    for c in range(left_ref.shape[0]):
        left_ref[c] = left_record
    pieces = []
    for t in range(factor // per):
        tile = right_rows[pl.ds(t * per, seqs, stride=factor), :] * keep
        for m in range(1, per):
            piece = right_rows[pl.ds(t * per + m, seqs, stride=factor), :] * keep
            tile = tile + turn(piece, m * res)
        pieces.append(tile)
    record = jnp.concatenate(pieces + [keep], axis=1).astype(bf16)
    for c in range(right_ref.shape[0]):
        right_ref[c] = record


def pair_kernel(
    parity_ref, rec_ref, other_ref, cot_ref, proj_ref, back_ref, send_ref, grad_ref,
    left_all, right_all, outer_all, adjoint_all, pulled_all, proj_rows, proj_all,
):
    shards, seqs, record = other_ref.shape
    blocks = 2
    even = parity_ref[0] == 0
    all_seqs = shards * seqs
    res = cot_ref.shape[0]
    cols = cot_ref.shape[1]
    wide = send_ref.shape[2]
    factor = wide // res
    pairs = lanes // cols
    sets = factor // pairs
    half = cols // blocks
    lane = lane_index((all_seqs, lanes))

    def left_tile(t):
        at = record + t * lanes
        return rec_ref[:, :, at : at + lanes].astype(f32).reshape(all_seqs, lanes)

    def right_tiles(t):
        own = rec_ref[:, :, t * lanes : (t + 1) * lanes].astype(f32).reshape(all_seqs, lanes)
        other = other_ref[:, :, t * lanes : (t + 1) * lanes].astype(f32).reshape(all_seqs, lanes)
        return jnp.where(even, own, other), jnp.where(even, other, own)

    proj_rows[...] = proj_ref[...].astype(f32)
    for n in range(sets):
        for k in range(pairs):
            proj_all[n * factor : (n + 1) * factor, k * lanes : (k + 1) * lanes] = proj_rows[
                pl.ds(n * pairs + k, factor, stride=factor), :
            ].astype(bf16)
    for t in range(wide // lanes):
        left_all[:, t * lanes : (t + 1) * lanes] = left_tile(t).astype(bf16)
    for t in range(wide // lanes):
        a, b = right_tiles(t)
        first = jnp.where(
            lane < 32, a, jnp.where(lane < 64, turn(b, 32), jnp.where(lane < 96, turn(a, 32), turn(b, 64)))
        )
        second = jnp.where(
            lane < 32, turn(a, 64), jnp.where(lane < 64, turn(b, 96), jnp.where(lane < 96, turn(a, 96), b))
        )
        right_all[:, 2 * t * lanes : (2 * t + 1) * lanes] = first.astype(bf16)
        right_all[:, (2 * t + 1) * lanes : (2 * t + 2) * lanes] = second.astype(bf16)
    last = wide // lanes
    keep_rows = left_tile(last).astype(bf16)
    a, b = right_tiles(last)
    keep_cols = (a + turn(b, half)).astype(bf16)
    count = first_first(keep_cols, keep_rows)[:cols]
    inverse = 1.0 / jnp.maximum(count, 1.0)
    nothing = jnp.zeros((cols, lanes), bf16)
    for i in range(res):
        scaled = (cot_ref[i].astype(f32) * inverse[:, i : i + 1]).astype(bf16)
        at = i * lanes
        for k in range(pairs):
            for m in range(pairs):
                adjoint_all[at + k * cols : at + (k + 1) * cols, m * lanes : (m + 1) * lanes] = (
                    scaled if k == m else nothing
                )
    step = 256 // factor
    for c in range(res // step):
        outer = first_first(left_all[:, c * step * factor : (c + 1) * step * factor], right_all[...])
        for i in range(step):
            at = (c * step + i) * lanes
            for n in range(sets):
                outer_all[n * factor : (n + 1) * factor, at : at + lanes] = outer[
                    i * factor : (i + 1) * factor, n * lanes : (n + 1) * lanes
                ].astype(bf16)
        pulled = last_last(proj_all[...], adjoint_all[c * step * lanes : (c + 1) * step * lanes, :])
        for i in range(step):
            at = (c * step + i) * factor
            for n in range(sets):
                pulled_all[at : at + factor, n * lanes : (n + 1) * lanes] = pulled[
                    n * factor : (n + 1) * factor, i * lanes : (i + 1) * lanes
                ].astype(bf16)
    grad_ref[...] = plain(outer_all[...], adjoint_all[...]).astype(bf16)
    grad_left = last_last(right_all[...], pulled_all[...])
    grad_right = plain(left_all[...], pulled_all[...])

    def put(ref, at, values):
        ref[:, :, at : at + lanes] = values.reshape(shards, seqs, lanes).astype(bf16)

    for t in range(wide // lanes):
        put(back_ref, wide + t * lanes, grad_left[:, t * lanes : (t + 1) * lanes])
        a = grad_right[:, 2 * t * lanes : (2 * t + 1) * lanes]
        b = grad_right[:, (2 * t + 1) * lanes : (2 * t + 2) * lanes]
        first = jnp.where(
            lane < 32, a, jnp.where(lane < 64, turn(a, 96), jnp.where(lane < 96, turn(b, 64), turn(b, 32)))
        )
        second = jnp.where(
            lane < 32, turn(a, 96), jnp.where(lane < 64, turn(a, 64), jnp.where(lane < 96, turn(b, 32), b))
        )
        put(back_ref, t * lanes, jnp.where(even, first, second))
        put(send_ref, t * lanes, jnp.where(even, second, first))


def chunk_rows(rows, features, hidden, factor, pair_width, chunks):
    sizes = (
        features * hidden // chunks // lanes,
        hidden * features // chunks // lanes,
        factor * factor * pair_width // chunks // lanes,
        2 * factor * features // chunks // lanes,
    )
    starts = [0]
    for size in sizes:
        starts.append(starts[-1] + size)
    return starts


def backward_kernel(
    core_ref, left_ref, right_ref, keep_ref, x_ref, cot_ref, scale_in_ref, w_in_ref, w_mid_ref,
    scale_out_ref, twin_ref, grad_ref, out_ref, own_ref, send_ref, left_rows, right_rows, chunks_ref,
):
    seqs = keep_ref.shape[0]
    rows, features = cot_ref.shape
    res = rows // seqs
    factor = twin_ref.shape[0] // 2
    group = lanes // factor
    per = lanes // res
    cols = own_ref.shape[0]
    chunks = 2 * cols
    units = w_in_ref.shape[1]
    pair_width = lanes
    starts = chunk_rows(rows, features, units, factor, pair_width, chunks)
    keep = keep_ref[...]
    lane_small = lane_index((seqs, lanes))
    normed_in, hidden, slope, hat_in, inv_in, hat_out, inv_out, normed_out = transition(
        x_ref[...].astype(f32), scale_in_ref[...], w_in_ref, scale_out_ref[...], w_mid_ref, True,
    )
    half = res * factor
    for t in range(res // group):
        tile = jnp.sum(left_ref[:, :, half + t * lanes : half + (t + 1) * lanes].astype(f32), axis=0)
        for m in range(group):
            piece = jnp.where(lane_small < factor, turn(tile, -m * factor), 0.0)
            left_rows[pl.ds(t * group + m, seqs, stride=res), :] = piece
    for t in range(factor // per):
        tile = jnp.sum(right_ref[:, :, t * lanes : (t + 1) * lanes].astype(f32), axis=0)
        for m in range(per):
            right_rows[pl.ds(t * per + m, seqs, stride=factor), :] = turn(tile, -m * res) * keep
    tiles = []
    for h in range(rows // lanes):
        tile = right_rows[h * per * factor : (h * per + 1) * factor, :]
        for m in range(1, per):
            at = (h * per + m) * factor
            tile = tile + turn(right_rows[at : at + factor, :], m * res)
        tiles.append(tile)
    turned = jnp.concatenate(tiles, axis=1)
    turned = jnp.concatenate(
        [jnp.zeros((factor, rows), f32), turned, jnp.zeros((lanes - 2 * factor, rows), f32)], axis=0
    )
    grad_proj = (left_rows[...] * keep_column(keep, seqs, res) + jnp.transpose(turned)).astype(bf16)
    twin = twin_ref[...]
    twin = jnp.concatenate([twin, jnp.zeros((lanes - 2 * factor, features), bf16)], axis=0)
    operand_adjoint = first_first(grad_proj, normed_out)
    rescaled = plain(grad_proj, twin)
    product_adjoint = jnp.sum(rescaled * hat_out, axis=0, keepdims=True)
    combined = cot_ref[...].astype(f32) + standardizer_adjoint(
        rescaled * scale_out_ref[...], hat_out, inv_out
    )
    mixed_half = combined.astype(bf16)
    grad_hidden = last_last(mixed_half, w_mid_ref[...])
    grad_pre = (slope * grad_hidden).astype(bf16)
    grad_in = last_last(grad_pre, w_in_ref[...])
    scale_adjoint = jnp.sum(grad_in * hat_in, axis=0, keepdims=True)
    out_ref[...] = (
        combined + standardizer_adjoint(grad_in * scale_in_ref[...], hat_in, inv_in)
    ).astype(bf16)
    hidden_adjoint = first_first(hidden, mixed_half)
    expansion_adjoint = first_first(normed_in, grad_pre)
    split = features // lanes

    def put(k, at, values):
        chunks_ref[k // cols, k % cols, at : at + values.shape[0], :] = values.astype(bf16)

    unit_step = units // chunks
    for k in range(chunks):
        put(k, starts[0], expansion_adjoint[:, k * unit_step : (k + 1) * unit_step])
        for m in range(split):
            put(k, starts[1] + m * unit_step,
                hidden_adjoint[k * unit_step : (k + 1) * unit_step, m * lanes : (m + 1) * lanes])
        height = grad_ref.shape[0] // chunks
        for m in range(grad_ref.shape[1] // lanes):
            put(k, starts[2] + m * height, grad_ref[k * height : (k + 1) * height, m * lanes : (m + 1) * lanes])
        height = 2 * factor // chunks
        tail = [
            operand_adjoint[k * height : (k + 1) * height, m * lanes : (m + 1) * lanes] for m in range(split)
        ]
        row = lax.broadcasted_iota(jnp.int32, (8, lanes), 0)
        extra = jnp.zeros((8, lanes), f32)
        if k == 0:
            for n, vector in enumerate((scale_adjoint, product_adjoint)):
                for m in range(split):
                    extra = jnp.where(row == n * split + m, vector[:, m * lanes : (m + 1) * lanes], extra)
        rest = chunks_ref.shape[2] - starts[4] - 8
        block = jnp.concatenate(tail + [extra, jnp.zeros((rest, lanes), f32)], axis=0)
        put(k, starts[3], block)
    core = core_ref[0]
    own_ref[...] = chunks_ref[core]
    send_ref[...] = chunks_ref[1 - core]


def final_kernel(
    core_ref, half_ref, other_ref, grad_ref, twin_ref, w_in_ref, w_mid_ref, scale_ref, product_ref
):
    cols = half_ref.shape[0]
    chunks = 2 * cols
    features, units = w_in_ref.shape
    factor = twin_ref.shape[0] // 2
    starts = chunk_rows(0, features, units, factor, lanes, chunks)
    split = features // lanes
    unit_step = units // chunks
    core = core_ref[0]
    height = factor * factor // 2 // chunks

    def read(k, at, size):
        return jnp.where(
            core == k // cols,
            half_ref[k % cols, at : at + size, :].astype(f32),
            other_ref[k % cols, at : at + size, :].astype(f32),
        )

    for k in range(chunks):
        span = slice(k * unit_step, (k + 1) * unit_step)
        w_in_ref[:, span] = read(k, starts[0], features)
        for m in range(split):
            w_mid_ref[span, m * lanes : (m + 1) * lanes] = read(k, starts[1] + m * unit_step, unit_step)
    for k in range(chunks):
        for m in range(2):
            block = read(k, starts[2] + m * height, height)
            for n in range(height // factor):
                q = 2 * (k * (height // factor) + n) + m
                grad_ref[pl.ds(q, factor, stride=factor), :] = block[n * factor : (n + 1) * factor]
    tall = 2 * factor // chunks
    for k in range(chunks):
        block = read(k, starts[3], starts[4] - starts[3])
        for m in range(split):
            twin_ref[k * tall : (k + 1) * tall, m * lanes : (m + 1) * lanes] = block[m * tall : (m + 1) * tall]
    extra = read(0, starts[4], 8)
    for n, ref in enumerate((scale_ref, product_ref)):
        for m in range(split):
            ref[:, m * lanes : (m + 1) * lanes] = extra[n * split + m : n * split + m + 1]


def call(kernel, outs, scratch, *args, scalars=0):
    specs = [pl.BlockSpec(memory_space=pltpu.SMEM)] * scalars
    specs += [pl.BlockSpec(memory_space=pltpu.VMEM)] * (len(args) - scalars)
    return pl.pallas_call(
        kernel,
        out_shape=[jax.ShapeDtypeStruct(s, d) for s, d in outs],
        in_specs=specs,
        out_specs=[pl.BlockSpec(memory_space=pltpu.VMEM)] * len(outs),
        scratch_shapes=[pltpu.VMEM(s, d) for s, d in scratch],
        interpret=INTERPRET,
    )(*args)


def exchanged(parts, axis, groups=None):
    return lax.all_to_all(
        parts, axis, split_axis=0, concat_axis=0, axis_index_groups=groups, tiled=True
    )


def copies(own, axis, groups):
    return exchanged(jnp.broadcast_to(own, (len(groups[0]),) + own.shape), axis, groups)


def per_device(
    saved_alignment,
    homolog_existence,
    amino_existence,
    couple_delta_adjoint,
    feedforward_adjoint,
    feedforward_scale,
    expansion_matrix,
    contraction_matrix,
    product_scale_vector,
    twin_operand_matrix,
    couple_projection_matrix,
):
    seqs, res, features = saved_alignment.shape
    units = expansion_matrix.shape[1]
    factor = twin_operand_matrix.shape[1] // 2
    pair_width = couple_projection_matrix.shape[1]
    rows = seqs * res
    row_devices, cols, cores = (lax.axis_size(a) for a in ("row", "col", "sub"))
    shards = cols * cores
    blocks = row_devices // shards
    col_res = couple_delta_adjoint.shape[1]
    all_seqs = seqs * shards
    wide = res * factor
    assert (factor, res, blocks, cores, pair_width) == (32, 32, 2, 2, lanes)
    assert col_res == blocks * res and features == 2 * lanes and units == shards * lanes
    x = saved_alignment.reshape(rows, features)
    scale_in = feedforward_scale.reshape(1, features)
    scale_out = product_scale_vector.reshape(1, features)
    twin = twin_operand_matrix.T
    record = wide + lanes
    keep, right, left = call(
        forward_kernel,
        [
            ((seqs, lanes), f32),
            ((row_devices // 2, seqs, record), bf16),
            ((shards, seqs, record), bf16),
        ],
        [
            ((rows, lanes), f32),
            ((seqs * factor, lanes), f32),
        ],
        x, homolog_existence, amino_existence.reshape(1, res), scale_in, expansion_matrix,
        contraction_matrix, scale_out, twin,
    )
    alike = [list(range(b, row_devices, 2)) for b in range(2)]
    swap_rows = [(i, i ^ 1) for i in range(row_devices)]
    parity = (lax.axis_index("row") % 2).reshape(1)
    right = exchanged(right, "row", alike)
    records = exchanged(
        jnp.concatenate([right, left], axis=2), ("col", "sub")
    )
    other = lax.ppermute(records[:, :, :record], "row", swap_rows)
    core = lax.axis_index("sub").reshape(1)
    other, parity, core = lax.optimization_barrier((other, parity, core))
    pairs = lanes // col_res
    sets = factor // pairs
    back, send, result_adjoint = call(
        pair_kernel,
        [
            ((shards, seqs, 2 * wide), bf16),
            ((shards, seqs, wide), bf16),
            ((sets * factor, pairs * lanes), bf16),
        ],
        [
            ((all_seqs, wide), bf16),
            ((all_seqs, col_res * factor), bf16),
            ((sets * factor, res * lanes), bf16),
            ((res * lanes, pairs * lanes), bf16),
            ((res * factor, sets * lanes), bf16),
            ((factor * factor, lanes), f32),
            ((sets * factor, pairs * lanes), bf16),
        ],
        parity, records, other, couple_delta_adjoint, couple_projection_matrix,
        scalars=1,
    )
    paired = jnp.pad(lax.ppermute(send, "row", swap_rows), ((0, 0), (0, 0), (0, wide)))
    back = exchanged((back.astype(f32) + paired.astype(f32)).astype(bf16), ("col", "sub"))
    right_back = exchanged(back[:, :, :wide], "row", alike)
    starts = chunk_rows(rows, features, units, factor, pair_width, shards)
    lines = -(-(starts[4] + 8) // (2 * row_devices)) * 2 * row_devices
    start_adjoint, own, send = call(
        backward_kernel,
        [
            ((rows, features), bf16),
            ((cols, lines, lanes), bf16),
            ((cols, lines, lanes), bf16),
        ],
        [
            ((rows, lanes), f32),
            ((seqs * factor, lanes), f32),
            ((cores, cols, lines, lanes), bf16),
        ],
        core, back, right_back, keep, x, feedforward_adjoint.reshape(rows, features), scale_in,
        expansion_matrix, contraction_matrix, scale_out, twin, result_adjoint,
        scalars=1,
    )
    swap = [(0, 1), (1, 0)]
    half = (own.astype(f32) + lax.ppermute(send, "sub", swap).astype(f32)).astype(bf16)
    near = [
        [(2 * m + b) * cols + c for c in range(cols) for b in range(2)] for m in range(row_devices // 2)
    ]
    half = exchanged(half.reshape(2 * cols, lines // 2, lanes), ("row", "col"), near)
    half = half.astype(f32).sum(axis=0).astype(bf16)
    half = exchanged(half.reshape(row_devices // 2, -1, 2, lanes), "row", alike)
    half = half.astype(f32).sum(axis=0).astype(bf16)
    half = copies(half, "row", alike).reshape(lines // 2, lanes)
    half = copies(half, ("row", "col"), near).reshape(cols, lines, lanes)
    other = lax.ppermute(half, "sub", swap)
    grads = call(
        final_kernel,
        [
            ((factor * factor, pair_width), f32),
            ((2 * factor, features), f32),
            ((features, units), f32),
            ((units, features), f32),
            ((1, features), f32),
            ((1, features), f32),
        ],
        [],
        core, half, other,
        scalars=1,
    )
    return (
        start_adjoint.reshape(seqs, res, features),
        grads[0],
        grads[1].T,
        grads[2],
        grads[3],
        grads[4].reshape(features),
        grads[5].reshape(features),
    )


def solution(mesh):
    return jax.shard_map(
        per_device,
        mesh=mesh,
        in_specs=(
            P(("col", "sub"), ("groups", "row"), None),
            P(("col", "sub"), ("groups", "row")),
            P(("groups", "row")),
            P(("groups", "row"), ("col", "sub"), None),
            P(("col", "sub"), ("groups", "row"), None),
            P(),
            P(),
            P(),
            P(),
            P(),
            P(),
        ),
        out_specs=(
            P(("col", "sub"), ("groups", "row"), None),
            P("groups", None),
            P("groups", None),
            P("groups", None),
            P("groups", None),
            P("groups"),
            P("groups"),
        ),
        check_vma=False,
    )
```
